256 devices in a mesh: fsdp: 32 (over z, y), rep: 8 (over x, core).
Axes of the slice: x: 4, y: 4, z: 8, core: 2. Of those that a mesh axis runs over, the one named last changes fastest.
Arguments:
- hidden: bfloat16 [65536, 2048], P(('fsdp', 'rep')), may hold values from -6 to 6
- attn_gain: bfloat16 [2048], P(('fsdp', 'rep')), may hold values from 0.25 to 1.75
- w_query: bfloat16 [2048, 2048], P(('fsdp', 'rep')), as said below
- w_key: bfloat16 [2048, 512], P(('fsdp', 'rep')), as said below
- w_value: bfloat16 [2048, 512], P(('fsdp', 'rep')), may hold values from -0.125 to 0.125
- w_out: bfloat16 [2048, 2048], P(None, ('fsdp', 'rep')), may hold values from -0.125 to 0.125
Outputs:
- mixed: bfloat16 [65536, 2048], P(('fsdp', 'rep'))
The draws below stay inside these ranges and needn't reach their ends.
Inputs may be any that keep to these rules, and one draw needn't show every extreme that they name: `w_query`: entries of order 2048^(-1/2). `w_key`: entries of order 2048^(-1/2) times a factor up to twenty.
All inputs are finite; a program needn't handle non-finite values.
Results may differ from the reference program's by a relative error of at most 0.012.
The reference program's roundings to bfloat16 on the way (of `normed`, `probs` and `context`) count: a program that leaves them out, or rounds other values in their place, can miss the bound.
Values may be sent and summed in bfloat16 or wider, within the bound.
A program may use at most 64 MiB of HBM per device.

```python
import math
import jax
import jax.numpy as jnp
from jax import lax

D = 2048
HEADS = 32
KV_HEADS = 8
HD = 64
TOK_DEV = 256
TOKENS = 65536
N_FSDP = 32
N_REP = 8


def shared_base(key):
    return jax.random.normal(jax.random.fold_in(key, 7), (D, KV_HEADS, 1, HD), jnp.float32) / math.sqrt(D)


def draw_w_query(key, part):
    group = HEADS // KV_HEADS
    others = jax.random.normal(jax.random.fold_in(key, 11), (D, KV_HEADS, group, HD), jnp.float32) / math.sqrt(D)
    joined = jnp.concatenate([shared_base(key), others[:, :, 1:, :]], axis=2)
    return joined.reshape(D, HEADS * HD).astype(jnp.bfloat16)


def draw_w_key(key, part):
    noise = jax.random.normal(jax.random.fold_in(key, 13), (D, KV_HEADS * HD), jnp.float32) / math.sqrt(D)
    result = noise
    return result.astype(jnp.bfloat16)


def block_levels(stream_key, extent, shards, least, high):
    def one(dim, parts):
        draws = jax.random.uniform(jax.random.fold_in(jax.random.fold_in(stream_key, 6), dim), (parts,), jnp.float32, least / len(shards), high / len(shards))
        return jnp.repeat(jnp.exp(draws), extent[dim] // parts).reshape((-1,) + (1,) * (len(extent) - dim - 1))

    level = one(*shards[0])
    for cut in shards[1:]:
        level = level * one(*cut)
    return level


def normal_values(key, extent, spread, most, split=(), held_as=jnp.bfloat16):
    values = jax.random.normal(key, extent, jnp.float32) * spread
    if len(split) > 0:
        values = block_levels(key, extent, split, -0.22, 0.18) * values
    return jnp.clip(values, min=-most, max=most).astype(held_as)


def setup_inputs(seed: int = 0) -> dict:
    streams_of = jax.random.split(jax.random.key(seed), 7)
    return {
        "hidden": normal_values(streams_of[0], (TOKENS, D), 1.0, 6.0, ((0, 256),)),
        "attn_gain": jnp.clip(1.0 + 0.15 * jax.random.normal(streams_of[1], (D,), jnp.float32), 0.25, 1.75).astype(jnp.bfloat16),
        "w_query": draw_w_query(jax.random.fold_in(streams_of[6], 71), 0),
        "w_key": draw_w_key(jax.random.fold_in(streams_of[6], 71), 0),
        "w_value": normal_values(streams_of[4], (D, KV_HEADS * HD), D ** -0.5, 0.125, ((0, 256),)),
        "w_out": normal_values(streams_of[5], (HEADS * HD, D), (HEADS * HD) ** -0.5, 0.125, ((1, 256),)),
    }


rope_base = 500000.0
norm_eps = 1e-05

def rope_tables(tokens, head_dim):
    position = jnp.arange(tokens, dtype=jnp.float32)
    freq = rope_base ** (-(jnp.arange(head_dim // 2, dtype=jnp.float32) * 2.0) / head_dim)
    angle = position[:, None] * freq[None, :]
    cos_table = jnp.concatenate([jnp.cos(angle), jnp.cos(angle)], axis=-1)
    sin_table = jnp.concatenate([jnp.sin(angle), jnp.sin(angle)], axis=-1)
    return (cos_table, sin_table)

def rotate(tensor, cos_table, sin_table):
    half = tensor.shape[-1] // 2
    turned = jnp.concatenate([-tensor[..., half:], tensor[..., :half]], axis=-1)
    return tensor * cos_table + turned * sin_table

def reference(hidden, attn_gain, w_query, w_key, w_value, w_out):
    group = HEADS // KV_HEADS
    cos_table, sin_table = rope_tables(TOK_DEV, HD)
    causal = jnp.arange(TOK_DEV)[:, None] >= jnp.arange(TOK_DEV)[None, :]

    def one_sequence(block):
        x_float = block.astype(jnp.float32)
        inv_rms = lax.rsqrt(lax.optimization_barrier(jnp.mean(x_float * x_float, axis=-1, keepdims=True)) + norm_eps)
        normed = (x_float * inv_rms * attn_gain.astype(jnp.float32)[None, :]).astype(jnp.bfloat16)
        queries = jnp.dot(normed, w_query, preferred_element_type=jnp.float32)
        keys_raw = jnp.dot(normed, w_key, preferred_element_type=jnp.float32)
        values_raw = jnp.dot(normed, w_value, preferred_element_type=jnp.float32)
        queries = queries.reshape(TOK_DEV, KV_HEADS, group, HD)
        keys_raw = keys_raw.reshape(TOK_DEV, KV_HEADS, HD)
        values_bf = values_raw.reshape(TOK_DEV, KV_HEADS, HD).astype(jnp.bfloat16)
        rope_queries = rotate(queries, cos_table[:, None, None, :], sin_table[:, None, None, :]).astype(jnp.bfloat16)
        rope_keys = rotate(keys_raw, cos_table[:, None, :], sin_table[:, None, :]).astype(jnp.bfloat16)
        scores = jnp.einsum('qkgd,skd->kgqs', rope_queries.astype(jnp.float32), rope_keys.astype(jnp.float32)) * HD ** (-0.5)
        scores = jnp.where(causal[None, None, :, :], scores, -1e+30)
        top = lax.optimization_barrier(jnp.max(scores, axis=-1, keepdims=True))
        expo = jnp.exp(scores - top)
        probs = (expo / lax.optimization_barrier(jnp.sum(expo, axis=-1, keepdims=True))).astype(jnp.bfloat16)
        context = jnp.einsum('kgqs,skd->qkgd', probs.astype(jnp.float32), values_bf.astype(jnp.float32))
        context = context.reshape(TOK_DEV, HEADS * HD).astype(jnp.bfloat16)
        return (x_float + jnp.dot(context, w_out, preferred_element_type=jnp.float32)).astype(jnp.bfloat16)
    blocks = hidden.reshape(N_FSDP * N_REP, TOK_DEV, D)
    return lax.map(one_sequence, blocks).reshape(TOKENS, D)
```

```python
import math

import jax
import jax.numpy as jnp
import numpy as np
from jax import lax
from jax.experimental import pallas as pl
from jax.experimental.pallas import tpu as pltpu
from jax.sharding import PartitionSpec as P

HD = 64
SEQ = 256
D = 2048
ROPE_BASE = 500000.0
NORM_EPS = 1e-05
MESH = pl.DeviceIdType.MESH

RING = {"x": 4, "y": 4, "z": 8}
ORDER = {"X": "zyx", "Y": "zxy", "Z": "xyz", "G": "xyz"}
LANES = {"X": {"p": 512, "o": 384}, "Y": {"p": 512, "o": 256}, "Z": {"p": 512, "o": 384}, "G": {"g": 32}}
WO_AT = {"X": 0, "Y": 384, "Z": 640}
RATE, LATENCY, ISSUE, BEGIN = 46.6e3, 1.9, 0.1, 4.0


def ring_steps(n, cut):
    for step in range(1, n // 2 + 1):
        for way in (1, -1):
            halves = (0, 1) if way > 0 else (1, 0)
            if step == n // 2:
                yield step, way, halves[:1]
            else:
                yield step, way, halves if cut else (None,)


def list_copies():
    copies, index = [], {}

    def add(key, size, needs):
        index[key] = len(copies)
        copies.append((key, size, [index[n] for n in needs]))

    for name in ORDER:
        first, second, last = ORDER[name]
        lanes = LANES[name]
        got = {(ring, part): [] for ring in range(3) for part in lanes}
        for ring, (axis, blocks) in enumerate(((first, 1), (second, RING[first]), (last, RING[first] * RING[second]))):
            n = RING[axis]
            for part in lanes:
                for step, way, halves in ring_steps(n, ring == 2 and name != "G"):
                    for half in halves:
                        if ring == 0 and name != "G":
                            if step == n // 2 and (part == "p") != (way > 0):
                                continue
                            half = None
                        key = (name, ring, part, step, way, half)
                        if step > 1:
                            before = (name, ring, part, step - 1, way, half)
                            needs = [before if before in index else before[:5] + (None,)]
                        else:
                            needs = got[ring - 1, part] if ring else []
                        size = blocks * lanes[part] * 32 / (1 if half is None else 2)
                        add(key, size, needs)
                        got[ring, part].append(key)
    return copies


def arrange(copies):
    come, free, order = {}, {}, []
    left = set(range(len(copies)))

    def rank(i):
        name, ring, part, step, way, half = copies[i][0]
        return ("gpo".index(part), ring, step, i)

    while left:
        best = None
        ready = {}
        for i in left:
            if all(n in come for n in copies[i][2]):
                key = copies[i][0]
                at = max([come[n] for n in copies[i][2]] + [BEGIN]) + ISSUE
                ready.setdefault((ORDER[key[0]][key[1]], key[4]), []).append((at, i))
        for link in sorted(ready):
            begin = max(free.get(link, 0.0), min(ready[link])[0])
            pick = min((i for at, i in ready[link] if at <= begin + 1e-9), key=rank)
            if best is None or (begin, pick) < best[:2]:
                best = (begin, pick, link)
        begin, pick, link = best
        free[link] = begin + copies[pick][1] / RATE
        come[pick] = free[link] + LATENCY
        left.remove(pick)
        order.append((begin, pick))
    return order, come


COPIES = list_copies()
SENT, COME = arrange(COPIES)
PART = {}
for number, (copy_key, _, _) in enumerate(COPIES):
    PART.setdefault((copy_key[0], copy_key[2]), []).append(number)


def dot(a, b):
    return lax.dot_general(a, b, (((1,), (0,)), ((), ())), preferred_element_type=jnp.float32)


def dot_t(a, b):
    return lax.dot_general(a, b, (((1,), (1,)), ((), ())), preferred_element_type=jnp.float32)


def kernel(
    hidden, gain, wq, wk, wv, wo, cos, sin, out,
    sx, sy, sz, sg, xs, normed, q_all, k_lo, k_hi, v_lo, v_hi, ctx, mine, gone, come,
    local, away, here, sent, got, out_sent, out_got,
):
    f, r = lax.axis_index("fsdp"), lax.axis_index("rep")
    at = {"z": f // 4, "y": f % 4, "x": r // 2}
    core = r % 2
    other = 1 - core
    partner = (f, at["x"] * 2 + other)

    def neighbour(axis, way):
        n = RING[axis]
        place = dict(at)
        place[axis] = (at[axis] + way + n) % n
        return (place["z"] * 4 + place["y"], place["x"] * 2 + core)

    barrier = pltpu.get_barrier_semaphore()
    peers = [partner] + [neighbour(axis, way) for axis in "xyz" for way in (1, -1)]
    for peer in peers:
        pl.semaphore_signal(barrier, inc=1, device_id=peer, device_id_type=MESH)

    buffers = {"X": sx, "Y": sy, "Z": sz, "G": sg}
    rows = pl.ds(pl.multiple_of(core * 8, 8), 8)
    own_rows = pl.ds(pl.multiple_of(core * SEQ, SEQ), SEQ)
    other_rows = pl.ds(pl.multiple_of(other * SEQ, SEQ), SEQ)

    def shares(t):
        def cut(ref, width, start, count):
            return ref.at[:, pl.ds(pl.multiple_of(t * width + start, 128), count)]

        for name, lane, source in (
            ("X", 0, cut(wq, 1024, 0, 512)),
            ("Y", 0, cut(wq, 1024, 512, 512)),
            ("Z", 0, cut(wk, 256, 0, 256)),
            ("Z", 256, cut(wv, 256, 0, 256)),
            ("X", 512, cut(wo, 1024, 0, 384)),
            ("Y", 512, cut(wo, 1024, 384, 256)),
            ("Z", 512, cut(wo, 1024, 640, 384)),
        ):
            a, b, c = (at[axis] for axis in ORDER[name])
            yield source, buffers[name].at[c, b, a, rows, pl.ds(lane, source.shape[1])]
        yield gain, sg.at[at["z"], at["y"], at["x"], core]
        yield hidden, xs.at[own_rows]

    starting = []
    for i, (source, target) in enumerate(shares(core)):
        starting.append(pltpu.make_async_copy(source, target, local.at[i]))
        starting[-1].start()
    tables = []
    pl.semaphore_wait(barrier, len(peers))
    for i, (source, target) in enumerate(shares(other)):
        copy = pltpu.make_async_remote_copy(
            src_ref=source, dst_ref=target, send_sem=away.at[i], recv_sem=here.at[i],
            device_id=partner, device_id_type=MESH,
        )
        copy.start()
        starting.append(copy)
    count = len(starting) // 2
    for copy in starting[: count - 1] + starting[count : 2 * count - 1]:
        copy.wait()

    def halves(n, half):
        return pl.ds(0, n) if half is None else pl.ds(half * (n // 2), n // 2)

    def transfer(i, moved):
        name, ring, part, step, way, half = COPIES[i][0]
        order = ORDER[name]
        a, b, c = (at[axis] for axis in order)
        axis = order[ring]
        n = RING[axis]
        block = (at[axis] - way * (step - 1 + moved) + n) % n
        if name == "G":
            tail = (halves(2, half),) if ring == 0 else ()
        else:
            start = 0 if part == "p" else LANES[name]["p"]
            tail = (slice(None), pl.ds(start, LANES[name][part]))
        if ring == 0:
            where = (c, b, block) + tail
        elif ring == 1:
            where = (c, block, halves(RING[order[0]], half)) + tail
        else:
            where = (block, halves(RING[order[1]], half)) + ((slice(None),) + tail if tail else ())
        ref = buffers[name].at[where]
        return pltpu.make_async_remote_copy(
            src_ref=ref, dst_ref=ref, send_sem=sent.at[i], recv_sem=got.at[i],
            device_id=neighbour(axis, way), device_id_type=MESH,
        )

    arrived = set()

    def await_copy(i):
        if i not in arrived:
            arrived.add(i)
            transfer(i, 1).wait_recv()

    def norm(lo):
        starting_rows = pl.ds(lo, 128)
        x = xs[starting_rows].astype(jnp.float32)
        scale = lax.rsqrt(jnp.mean(x * x, axis=-1, keepdims=True) + NORM_EPS)
        for tile in range(16):
            z, y = tile // 2, tile % 2 * 2
            weight = sg[z, y, 0, 0]
            for k in range(1, 16):
                weight = weight + sg[z, y + k // 8, k // 2 % 4, k % 2]
            lanes = slice(tile * 128, tile * 128 + 128)
            normed[starting_rows, lanes] = (x[:, lanes] * scale * weight).astype(jnp.bfloat16)

    lane = lax.broadcasted_iota(jnp.int32, (SEQ, 128), 1)

    def rope(t):
        turned = jnp.where(lane % 64 < 32, pltpu.roll(t, 96, 1), pltpu.roll(t, 32, 1))
        return t * cos[...] + turned * sin[...]

    def columns(name, lo, n):
        pieces = []
        for z in range(8):
            for y in range(4):
                for x in range(4):
                    place = {"x": x, "y": y, "z": z}
                    a, b, c = (place[axis] for axis in ORDER[name])
                    pieces.append(buffers[name][c, b, a, :, lo : lo + n])
        return jnp.concatenate(pieces, axis=0)

    def project_q(name, lo, start):
        t = dot(normed[...], columns(name, lo, 256))
        for s in range(2):
            for half in range(2):
                piece = rope(t[s * SEQ : s * SEQ + SEQ, half * 128 : half * 128 + 128])
                q_all[s * SEQ : s * SEQ + SEQ, start + half * 128 : start + half * 128 + 128] = (
                    piece * HD**-0.5
                ).astype(jnp.bfloat16)

    def project_kv(lo, turn, low, high):
        t = dot(normed[...], columns("Z", lo, 256))
        for s in range(2):
            for pair in range(2):
                piece = t[s * SEQ : s * SEQ + SEQ, pair * 128 : pair * 128 + 128]
                if turn:
                    piece = rope(piece)
                moved = pltpu.roll(piece, 64, 1)
                zero = jnp.zeros_like(piece)
                here_rows = slice(s * SEQ, s * SEQ + SEQ)
                for odd in range(2):
                    same, swapped = jnp.where(lane < 64, piece, zero), jnp.where(lane < 64, zero, moved)
                    if odd:
                        same, swapped = jnp.where(lane < 64, moved, zero), jnp.where(lane < 64, zero, piece)
                    low[2 * pair + odd, here_rows] = same.astype(jnp.bfloat16)
                    high[2 * pair + odd, here_rows] = swapped.astype(jnp.bfloat16)

    def attend(s, head):
        keys = (k_lo[head, s * SEQ : s * SEQ + SEQ], k_hi[head, s * SEQ : s * SEQ + SEQ])
        values = jnp.concatenate(
            [v_lo[head, s * SEQ : s * SEQ + SEQ], v_hi[head, s * SEQ : s * SEQ + SEQ]], axis=0
        )
        for pair in range(2):
            start = head * 256 + pair * 128
            for block in range(2):
                n = 128 * (block + 1)
                lo = s * SEQ + block * 128
                queries = q_all[lo : lo + 128, start : start + 128]
                probs = []
                for key in keys:
                    scores = dot_t(queries, key[:n])
                    ahead = lax.broadcasted_iota(jnp.int32, (128, n), 1) <= (
                        lax.broadcasted_iota(jnp.int32, (128, n), 0) + block * 128
                    )
                    scores = jnp.where(ahead, scores, -1e30)
                    expo = jnp.exp(scores - jnp.max(scores, axis=-1, keepdims=True))
                    probs.append((expo / jnp.sum(expo, axis=-1, keepdims=True)).astype(jnp.bfloat16))
                mixed = dot(probs[0], values[:n]) + dot(probs[1], values[SEQ : SEQ + n])
                ctx[lo : lo + 128, start : start + 128] = mixed.astype(jnp.bfloat16)

    def await_part(*parts):
        for part in parts:
            for i in PART[part]:
                await_copy(i)

    works = []

    def work(parts, cost, run, *args):
        ready = max(COME[i] for part in parts for i in PART[part])
        works.append((ready, cost, parts, run, args))

    def first_norm():
        starting[count - 1].wait()
        starting[2 * count - 1].wait()

    work([("G", "g")], 0.0, first_norm)
    for lo in range(0, 2 * SEQ, 128):
        work([("G", "g")], 0.6, norm, lo)
    work([("Z", "p")], 0.9, project_kv, 0, True, k_lo, k_hi)
    work([("Z", "p")], 0.9, project_kv, 256, False, v_lo, v_hi)
    for name, start in (("X", 0), ("Y", 512)):
        for lo in (0, 256):
            work([(name, "p")], 0.9, project_q, name, lo, start + lo)
    for name, heads in (("X", (0, 1)), ("Y", (2, 3))):
        for head in heads:
            for s in range(2):
                work([(name, "p"), ("Z", "p")], 1.0, attend, s, head)
    works.sort(key=lambda w: w[0])

    now = 0.0

    def do_work():
        nonlocal now
        ready, cost, parts, run, args = works.pop(0)
        await_part(*parts)
        run(*args)
        now = max(now, ready) + cost

    for begin, i in SENT:
        while works and max(works[0][0], now) + works[0][1] <= begin + 0.3:
            do_work()
        for j in COPIES[i][2]:
            await_copy(j)
        transfer(i, 0).start()
        now = max(now, begin)
    while works:
        do_work()

    for i in range(len(COPIES)):
        await_copy(i)

    def leaving(z):
        return pltpu.make_async_remote_copy(
            src_ref=gone.at[z], dst_ref=come.at[z], send_sem=out_sent.at[z], recv_sem=out_got.at[z],
            device_id=partner, device_id_type=MESH,
        )

    def context_of(chosen):
        return jnp.concatenate([ctx[chosen, :]], axis=0)

    for z in range(8):
        weights = []
        for name in "XYZ":
            lo, n = LANES[name]["p"], LANES[name]["o"]
            pieces = []
            for y in range(4):
                for x in range(4):
                    place = {"x": x, "y": y, "z": z}
                    a, b, c = (place[axis] for axis in ORDER[name])
                    pieces.append(buffers[name][c, b, a, :, lo : lo + n])
            weights.append(jnp.concatenate(pieces, axis=0))
        weights = jnp.concatenate(weights, axis=1)
        gone[z] = dot_t(ctx[other_rows, :], weights)
        leaving(z).start()
        mine[z] = dot_t(ctx[own_rows, :], weights)
    for z in range(8):
        lanes = slice(z * 256, z * 256 + 256)
        leaving(z).wait_recv()
        out[:, lanes] = (xs[own_rows, lanes].astype(jnp.float32) + (mine[z] + come[z])).astype(jnp.bfloat16)
    for z in range(8):
        leaving(z).wait_send()
    for i in range(len(COPIES)):
        transfer(i, 0).wait_send()


def rope_tables():
    position = np.arange(SEQ, dtype=np.float64)
    freq = ROPE_BASE ** (-(np.arange(HD // 2) * 2.0) / HD)
    angle = position[:, None] * freq[None, :]
    cos = np.tile(np.cos(angle), (1, 4))
    sin = np.tile(np.concatenate([-np.sin(angle), np.sin(angle)], axis=1), (1, 2))
    return cos.astype(np.float32), sin.astype(np.float32)


def body(hidden, gain, wq, wk, wv, w_out):
    cos, sin = rope_tables()
    device = lax.axis_index("fsdp") * 8 + lax.axis_index("rep")
    spread = jnp.tile(gain.astype(jnp.float32), 16)
    spread = jnp.where(jnp.arange(128) // 8 == device % 16, spread, 0.0)[None, :]
    vmem = pltpu.VMEM
    bf16, f32 = jnp.bfloat16, jnp.float32
    n = len(COPIES)
    dma = pltpu.SemaphoreType.DMA
    anywhere = pl.BlockSpec(memory_space=pl.ANY)
    inside = pl.BlockSpec(memory_space=pltpu.VMEM)
    return pl.pallas_call(
        kernel,
        out_shape=jax.ShapeDtypeStruct((SEQ, D), bf16),
        in_specs=[anywhere] * 6 + [inside] * 2,
        out_specs=inside,
        scratch_shapes=[
            vmem((4, 4, 8, 16, 896), bf16),
            vmem((4, 4, 8, 16, 768), bf16),
            vmem((8, 4, 4, 16, 896), bf16),
            vmem((8, 4, 4, 2, 1, 128), f32),
            vmem((2 * SEQ, D), bf16),
            vmem((2 * SEQ, D), bf16),
            vmem((2 * SEQ, 1024), bf16),
            vmem((4, 2 * SEQ, 128), bf16),
            vmem((4, 2 * SEQ, 128), bf16),
            vmem((4, 2 * SEQ, 128), bf16),
            vmem((4, 2 * SEQ, 128), bf16),
            vmem((2 * SEQ, 1024), bf16),
            vmem((8, SEQ, 256), f32),
            vmem((8, SEQ, 256), f32),
            vmem((8, SEQ, 256), f32),
            dma((9,)), dma((9,)), dma((9,)), dma((n,)), dma((n,)), dma((8,)), dma((8,)),
        ],
        compiler_params=pltpu.CompilerParams(
            collective_id=0, has_side_effects=True, vmem_limit_bytes=60 * 2**20
        ),
        name="attention_block",
    )(hidden, spread, wq, wk, wv, w_out.T, cos, sin)


def solution(mesh):
    rows = P(("fsdp", "rep"), None)
    placed = (rows, P(("fsdp", "rep")), rows, rows, rows, P(None, ("fsdp", "rep")))
    return jax.shard_map(body, mesh=mesh, in_specs=placed, out_specs=rows, check_vma=False)
```

```python
import math

import jax
import jax.numpy as jnp
import numpy as np
from jax import lax
from jax.experimental import pallas as pl
from jax.experimental.pallas import tpu as pltpu
from jax.sharding import PartitionSpec as P

HD = 64
SEQ = 256
D = 2048
ROPE_BASE = 500000.0
NORM_EPS = 1e-05
MESH = pl.DeviceIdType.MESH

RING = {"x": 4, "y": 4, "z": 8}
ORDER = {"X": "zyx", "Y": "zxy", "Z": "yxz", "G": "xyz"}
LANES = {"X": {"p": 512, "o": 384}, "Y": {"p": 512, "o": 256}, "Z": {"p": 512, "o": 384}, "G": {"g": 32}}
GROUPS = {8: ((0, 3), (3, 2), (5, 3)), 4: ((0, 1), (1, 2), (3, 1))}
RATE, LATENCY, ISSUE, BEGIN = 46.6e3, 2.2, 0.1, 4.0


def slot(n, step, way):
    return n - 1 if step == n // 2 else 2 * step - (way < 0 and step > 0)


def list_copies():
    copies, index = [], {}

    def go_round(prefix, axis, size, first, cut):
        n, made = RING[axis], []
        for step in range(1, n // 2 + 1):
            for way in (1, -1):
                halves = (0, 1) if way > 0 else (1, 0)
                for half in halves[:1] if step == n // 2 else halves if cut else (None,):
                    key = prefix + (step, way, half)
                    before = prefix + (step - 1, way, half)
                    if before not in index:
                        before = prefix + (step - 1, way, None)
                    needs = first if step == 1 else [before]
                    index[key] = len(copies)
                    copies.append((key, size / (1 if half is None else 2), [index[k] for k in needs]))
                    made.append(key)
        return made

    for name, (first, second, last) in ORDER.items():
        n = RING[first]
        for part, lanes in LANES[name].items():
            made = go_round((part, name, 0, (0, n)), first, lanes * 32, [], False)
            for group in GROUPS[n] if part == "p" else ((0, n),):
                needs = [k for k in made if group[0] <= slot(n, k[4], k[5]) < sum(group)]
                size = lanes * 32 * group[1]
                passed = go_round((part, name, 1, group), second, size, needs, False)
                go_round((part, name, 2, group), last, size * RING[second], passed, part == "o")
    return copies


def arrange(copies):
    come, free, order = {}, {}, []
    left = set(range(len(copies)))

    def rank(i):
        part, name, ring, group, step, way, half = copies[i][0]
        return (part != "g", ring == 2 and part == "o", ring, -step, i)

    while left:
        best = None
        ready = {}
        for i in left:
            if all(n in come for n in copies[i][2]):
                key = copies[i][0]
                at = max([come[n] for n in copies[i][2]] + [BEGIN]) + ISSUE
                ready.setdefault((ORDER[key[1]][key[2]], key[5]), []).append((at, i))
        for link in sorted(ready):
            begin = max(free.get(link, 0.0), min(ready[link])[0])
            pick = min((i for at, i in ready[link] if at <= begin + 1e-9), key=rank)
            if best is None or (begin, pick) < best[:2]:
                best = (begin, pick, link)
        begin, pick, link = best
        free[link] = begin + copies[pick][1] / RATE
        come[pick] = free[link] + LATENCY
        left.remove(pick)
        order.append((begin, pick))
    return order, come


COPIES = list_copies()
SENT, COME = arrange(COPIES)
PART = {}
for number, (copy_key, _, _) in enumerate(COPIES):
    PART.setdefault((copy_key[1], copy_key[0]), []).append(number)
FAR = [(0, 0), (1, 1), (1, -1), (2, 1), (2, -1), (3, 1), (3, -1), (4, 1)]
LAST = {}
for number, (copy_key, _, _) in enumerate(COPIES):
    if copy_key[:3] == ("o", "Z", 2):
        LAST.setdefault((copy_key[4], 1 if copy_key[4] == 4 else copy_key[5]), []).append(number)


def dot(a, b):
    return lax.dot_general(a, b, (((1,), (0,)), ((), ())), preferred_element_type=jnp.float32)


def dot_t(a, b):
    return lax.dot_general(a, b, (((1,), (1,)), ((), ())), preferred_element_type=jnp.float32)


def kernel(
    hidden, gain, wq, wk, wv, wo, cos_in, sin_in, out,
    px, py, pz, ox, oy, oz, sg, xs, cos, sin, normed, q_all, k_lo, k_hi, v_lo, v_hi,
    score, prob, ctx, acc, mine, gone, come,
    local, away, here, sent, got, out_sent, out_got,
):
    f, r = lax.axis_index("fsdp"), lax.axis_index("rep")
    at = {"z": f // 4, "y": f % 4, "x": r // 2}
    core = r % 2
    other = 1 - core
    partner = (f, at["x"] * 2 + other)

    def neighbour(axis, way):
        n = RING[axis]
        place = dict(at)
        place[axis] = (at[axis] + way + n) % n
        return (place["z"] * 4 + place["y"], place["x"] * 2 + core)

    barrier = pltpu.get_barrier_semaphore()
    peers = [partner] + [neighbour(axis, way) for axis in "xyz" for way in (1, -1)]
    for peer in peers:
        pl.semaphore_signal(barrier, inc=1, device_id=peer, device_id_type=MESH)

    buffers = {"Xp": px, "Yp": py, "Zp": pz, "Xo": ox, "Yo": oy, "Zo": oz, "Gg": sg}
    rows = pl.ds(pl.multiple_of(core * 8, 8), 8)
    own_rows = pl.ds(pl.multiple_of(core * SEQ, SEQ), SEQ)
    other_rows = pl.ds(pl.multiple_of(other * SEQ, SEQ), SEQ)

    def shares(t):
        def cut(ref, width, start, count):
            return ref.at[:, pl.ds(pl.multiple_of(t * width + start, 128), count)]

        for name, lane, source in (
            ("Xp", 0, cut(wq, 1024, 0, 512)),
            ("Yp", 0, cut(wq, 1024, 512, 512)),
            ("Zp", 0, cut(wk, 256, 0, 256)),
            ("Zp", 256, cut(wv, 256, 0, 256)),
            ("Xo", 0, cut(wo, 1024, 0, 384)),
            ("Yo", 0, cut(wo, 1024, 384, 256)),
            ("Zo", 0, cut(wo, 1024, 640, 384)),
        ):
            _, b, c = (at[axis] for axis in ORDER[name[0]])
            yield source, buffers[name].at[c, b, 0, rows, pl.ds(lane, source.shape[1])]
        yield gain, sg.at[at["z"], at["y"], 0, core]
        yield hidden, xs.at[own_rows]

    starting = []
    for i, (source, target) in enumerate(shares(core)):
        starting.append(pltpu.make_async_copy(source, target, local.at[i]))
        starting[-1].start()
    tables = [
        pltpu.make_async_copy(cos_in, cos, local.at[9]),
        pltpu.make_async_copy(sin_in, sin, local.at[10]),
    ]
    for copy in tables:
        copy.start()
    pl.semaphore_wait(barrier, len(peers))
    for i, (source, target) in enumerate(shares(other)):
        copy = pltpu.make_async_remote_copy(
            src_ref=source, dst_ref=target, send_sem=away.at[i], recv_sem=here.at[i],
            device_id=partner, device_id_type=MESH,
        )
        copy.start()
        starting.append(copy)
    count = len(starting) // 2
    for copy in starting[: count - 1] + starting[count : 2 * count - 1]:
        copy.wait()

    def halves(n, half):
        return pl.ds(0, n) if half is None else pl.ds(half * (n // 2), n // 2)

    def lane_half(n, half):
        first = (n // 128 + 1) // 2 * 128
        return pl.ds(0, n) if half is None else pl.ds(0, first) if half == 0 else pl.ds(first, n - first)

    def transfer(i):
        part, name, ring, group, step, way, half = COPIES[i][0]
        a, b, c = (at[axis] for axis in ORDER[name])
        axis = ORDER[name][ring]
        n = RING[axis]
        buffer = buffers[name + part]
        lanes = LANES[name][part]
        block = (at[axis] - way * (step - 1) + n) % n
        source = target = None
        if ring == 0:
            tail = (halves(2, half),) if part == "g" else (slice(None), lane_half(lanes, half))
            source = buffer.at[(c, b, slot(n, step - 1, way)) + tail]
            target = buffer.at[(c, b, slot(n, step, way)) + tail]
        elif ring == 1:
            slots = pl.ds(*group)
            if part == "g":
                source = target = buffer.at[c, block, halves(group[1], half)]
            else:
                source = target = buffer.at[c, block, slots, :, lane_half(lanes, half)]
        else:
            slots = pl.ds(*group)
            source = target = buffer.at[block, halves(RING[ORDER[name][1]], half), slots]
        return pltpu.make_async_remote_copy(
            src_ref=source, dst_ref=target, send_sem=sent.at[i], recv_sem=got.at[i],
            device_id=neighbour(axis, way), device_id_type=MESH,
        )

    def incoming(i):
        part, name, ring, group, step, way, half = COPIES[i][0]
        if ring == 0:
            return transfer(i)
        a, b, c = (at[axis] for axis in ORDER[name])
        axis = ORDER[name][ring]
        n = RING[axis]
        buffer = buffers[name + part]
        lanes = LANES[name][part]
        block = (at[axis] - way * step + n) % n
        if ring == 1 and part == "g":
            target = buffer.at[c, block, halves(group[1], half)]
        elif ring == 1:
            target = buffer.at[c, block, pl.ds(*group), :, lane_half(lanes, half)]
        else:
            target = buffer.at[block, halves(RING[ORDER[name][1]], half), pl.ds(*group)]
        return pltpu.make_async_remote_copy(
            src_ref=target, dst_ref=target, send_sem=sent.at[i], recv_sem=got.at[i],
            device_id=neighbour(axis, way), device_id_type=MESH,
        )

    arrived = set()

    def await_copy(i):
        if i not in arrived:
            arrived.add(i)
            incoming(i).wait_recv()

    def slots_of(axis):
        n = RING[axis]
        found = []
        for place in range(n):
            d = (place - at[axis] + n) % n
            found.append(jnp.where(d == 0, 0, jnp.where(d <= n // 2, 2 * d - 1, 2 * (n - d))))
        return found

    place_slots = {axis: slots_of(axis) for axis in "yz"}

    def norm(lo):
        chosen = pl.ds(lo, 128)
        x = xs[chosen].astype(jnp.float32)
        scale = lax.rsqrt(jnp.mean(x * x, axis=-1, keepdims=True) + NORM_EPS)
        for tile in range(16):
            z, y = tile // 2, tile % 2 * 2
            weight = sg[z, y, 0, 0]
            for k in range(1, 16):
                weight = weight + sg[z, y + k // 8, k // 2 % 4, k % 2]
            lanes = slice(tile * 128, tile * 128 + 128)
            normed[chosen, lanes] = (x[:, lanes] * scale * weight).astype(jnp.bfloat16)

    lane = lax.broadcasted_iota(jnp.int32, (SEQ, 128), 1)

    def rope(t):
        turned = jnp.where(lane % 64 < 32, pltpu.roll(t, 96, 1), pltpu.roll(t, 32, 1))
        return t * cos[...] + turned * sin[...]

    def features(name, z, lo, n):
        first, second, last = ORDER[name[0]]
        pieces = []
        for y in range(4):
            for x in range(4):
                place = {"x": x, "y": y, "z": z}
                pieces.append(
                    buffers[name][place[last], place[second], place_slots[first][place[first]], :, lo : lo + n]
                )
        return pieces

    def columns(name, lo, n):
        return jnp.concatenate([piece for z in range(8) for piece in features(name, z, lo, n)], axis=0)

    def project_q(name, lo, start):
        t = dot(normed[...], columns(name, lo, 256))
        for s in range(2):
            for half in range(2):
                piece = rope(t[s * SEQ : s * SEQ + SEQ, half * 128 : half * 128 + 128])
                q_all[s * SEQ : s * SEQ + SEQ, start + half * 128 : start + half * 128 + 128] = (
                    piece * HD**-0.5
                ).astype(jnp.bfloat16)

    def project_kv(lo, turn, low, high):
        t = dot(normed[...], columns("Zp", lo, 256))
        for s in range(2):
            for pair in range(2):
                piece = t[s * SEQ : s * SEQ + SEQ, pair * 128 : pair * 128 + 128]
                if turn:
                    piece = rope(piece)
                moved = pltpu.roll(piece, 64, 1)
                zero = jnp.zeros_like(piece)
                here_rows = slice(s * SEQ, s * SEQ + SEQ)
                for odd in range(2):
                    same, swapped = jnp.where(lane < 64, piece, zero), jnp.where(lane < 64, zero, moved)
                    if odd:
                        same, swapped = jnp.where(lane < 64, moved, zero), jnp.where(lane < 64, zero, piece)
                    low[2 * pair + odd, here_rows] = same.astype(jnp.bfloat16)
                    high[2 * pair + odd, here_rows] = swapped.astype(jnp.bfloat16)

    def attend(s, head):
        here_rows = slice(s * SEQ, s * SEQ + SEQ)
        keys = (k_lo[head, here_rows], k_hi[head, here_rows])
        values = jnp.concatenate([v_lo[head, here_rows], v_hi[head, here_rows]], axis=0)
        for pair in range(2):
            start = head * 256 + pair * 128
            for odd in range(2):
                score[2 * pair + odd] = dot_t(q_all[here_rows, start : start + 128], keys[odd])
        for unit in range(4):
            for block in range(4):
                n = 128 * (block // 2 + 1)
                chosen = slice(block * 64, block * 64 + 64)
                t = score[unit, chosen, :n]
                seen = lax.broadcasted_iota(jnp.int32, (64, n), 1) <= (
                    lax.broadcasted_iota(jnp.int32, (64, n), 0) + block * 64
                )
                t = jnp.where(seen, t, -1e30)
                expo = jnp.exp(t - jnp.max(t, axis=-1, keepdims=True))
                share = 1.0 / jnp.sum(expo, axis=-1, keepdims=True)
                prob[unit // 2, chosen, unit % 2 * SEQ : unit % 2 * SEQ + n] = (expo * share).astype(jnp.bfloat16)
        for pair in range(2):
            start = head * 256 + pair * 128
            ctx[here_rows, start : start + 128] = dot(prob[pair], values).astype(jnp.bfloat16)

    def mix_first(z):
        weights = jnp.concatenate(
            [
                jnp.concatenate(features("Xo", z, 0, 384), axis=0),
                jnp.concatenate(features("Yo", z, 0, 256), axis=0),
            ],
            axis=1,
        )
        acc[z] = dot_t(ctx[:, :640], weights)

    def chunk_of(k):
        step, way = FAR[k]
        return (at["z"] - way * step + 8) % 8

    def leaving(k):
        return pltpu.make_async_remote_copy(
            src_ref=gone.at[k], dst_ref=come.at[k], send_sem=out_sent.at[k], recv_sem=out_got.at[k],
            device_id=partner, device_id_type=MESH,
        )

    def mix_last(k):
        z = chunk_of(k)
        weights = jnp.concatenate(features("Zo", z, 0, 384), axis=0)
        gone[k] = acc[z, other_rows] + dot_t(ctx[other_rows, 640:], weights)
        mine[k] = acc[z, own_rows] + dot_t(ctx[own_rows, 640:], weights)
        leaving(k).start()

    works = []

    def work(parts, cost, run, *args, needs=()):
        needs = list(needs) + [i for part in parts for i in PART[part]]
        works.append((max(COME[i] for i in needs), cost, needs, run, args))

    def prepare():
        starting[count - 1].wait()
        starting[2 * count - 1].wait()
        for copy in tables:
            copy.wait()
        for pair in range(2):
            for odd in range(2):
                prob[pair, :128, odd * SEQ + 128 : odd * SEQ + SEQ] = jnp.zeros((128, 128), jnp.bfloat16)

    work([("G", "g")], 0.0, prepare)
    for lo in range(0, 2 * SEQ, 128):
        work([("G", "g")], 0.2, norm, lo)
    work([("Z", "p")], 0.8, project_kv, 0, True, k_lo, k_hi)
    work([("Z", "p")], 0.8, project_kv, 256, False, v_lo, v_hi)
    for name, start in (("X", 0), ("Y", 512)):
        for lo in (0, 256):
            work([(name, "p")], 0.8, project_q, name + "p", lo, start + lo)
    works[5:] = sorted(works[5:], key=lambda w: w[0])
    for name, heads in (("X", (0, 1)), ("Y", (2, 3))):
        for head in heads:
            for s in range(2):
                work([(name, "p"), ("Z", "p")], 1.0, attend, s, head)
    for z in range(8):
        work([("X", "o"), ("Y", "o")], 0.4, mix_first, z)
    for k in range(8):
        work([], 0.3, mix_last, k, needs=LAST[FAR[k]] if k else [i for i in PART["Z", "o"] if COPIES[i][0][2] < 2])

    now = 0.0

    def do_work():
        nonlocal now
        ready, cost, needs, run, args = works.pop(0)
        for i in needs:
            await_copy(i)
        run(*args)
        now = max(now, ready) + cost

    for begin, i in SENT:
        while works and max(works[0][0], now) + works[0][1] <= begin + 0.3:
            do_work()
        for j in COPIES[i][2]:
            await_copy(j)
        transfer(i).start()
        now = max(now, begin)
    while works:
        do_work()
    for i in range(len(COPIES)):
        await_copy(i)

    for k in range(8):
        lanes = pl.ds(pl.multiple_of(chunk_of(k) * 256, 256), 256)
        leaving(k).wait_recv()
        out[:, lanes] = (xs[own_rows, lanes].astype(jnp.float32) + (mine[k] + come[k])).astype(jnp.bfloat16)
    for k in range(8):
        leaving(k).wait_send()
    for i in range(len(COPIES)):
        transfer(i).wait_send()


def rope_tables():
    position = np.arange(SEQ, dtype=np.float64)
    freq = ROPE_BASE ** (-(np.arange(HD // 2) * 2.0) / HD)
    angle = position[:, None] * freq[None, :]
    cos = np.tile(np.cos(angle), (1, 4))
    sin = np.tile(np.concatenate([-np.sin(angle), np.sin(angle)], axis=1), (1, 2))
    return cos.astype(np.float32), sin.astype(np.float32)


def body(hidden, gain, wq, wk, wv, w_out):
    cos, sin = rope_tables()
    device = lax.axis_index("fsdp") * 8 + lax.axis_index("rep")
    spread = jnp.tile(gain.astype(jnp.float32), 16)
    spread = jnp.where(jnp.arange(128) // 8 == device % 16, spread, 0.0)[None, :]
    vmem = pltpu.VMEM
    bf16, f32 = jnp.bfloat16, jnp.float32
    n = len(COPIES)
    dma = pltpu.SemaphoreType.DMA
    anywhere = pl.BlockSpec(memory_space=pl.ANY)
    inside = pl.BlockSpec(memory_space=pltpu.VMEM)
    return pl.pallas_call(
        kernel,
        out_shape=jax.ShapeDtypeStruct((SEQ, D), bf16),
        in_specs=[anywhere] * 8,
        out_specs=inside,
        scratch_shapes=[
            vmem((4, 4, 8, 16, 512), bf16),
            vmem((4, 4, 8, 16, 512), bf16),
            vmem((8, 4, 4, 16, 512), bf16),
            vmem((4, 4, 8, 16, 384), bf16),
            vmem((4, 4, 8, 16, 256), bf16),
            vmem((8, 4, 4, 16, 384), bf16),
            vmem((8, 4, 4, 2, 1, 128), f32),
            vmem((2 * SEQ, D), bf16),
            vmem((SEQ, 128), f32),
            vmem((SEQ, 128), f32),
            vmem((2 * SEQ, D), bf16),
            vmem((2 * SEQ, 1024), bf16),
            vmem((4, 2 * SEQ, 128), bf16),
            vmem((4, 2 * SEQ, 128), bf16),
            vmem((4, 2 * SEQ, 128), bf16),
            vmem((4, 2 * SEQ, 128), bf16),
            vmem((4, SEQ, SEQ), f32),
            vmem((2, SEQ, 2 * SEQ), bf16),
            vmem((2 * SEQ, 1024), bf16),
            vmem((8, 2 * SEQ, 256), f32),
            vmem((8, SEQ, 256), f32),
            vmem((8, SEQ, 256), f32),
            vmem((8, SEQ, 256), f32),
            dma((11,)), dma((9,)), dma((9,)), dma((n,)), dma((n,)), dma((8,)), dma((8,)),
        ],
        compiler_params=pltpu.CompilerParams(
            collective_id=0, has_side_effects=True, vmem_limit_bytes=60 * 2**20
        ),
        name="attention_block",
    )(hidden, spread, wq, wk, wv, w_out.T, cos, sin)


def solution(mesh):
    rows = P(("fsdp", "rep"), None)
    placed = (rows, P(("fsdp", "rep")), rows, rows, rows, P(None, ("fsdp", "rep")))
    return jax.shard_map(body, mesh=mesh, in_specs=placed, out_specs=rows, check_vma=False)
```

```python
import math

import jax
import jax.numpy as jnp
import numpy as np
from jax import lax
from jax.experimental import pallas as pl
from jax.experimental.pallas import tpu as pltpu
from jax.sharding import PartitionSpec as P

HD = 64
SEQ = 256
D = 2048
ROPE_BASE = 500000.0
NORM_EPS = 1e-05
MESH = pl.DeviceIdType.MESH

RING = {"x": 4, "y": 4, "z": 8}
ORDER = {"X": "zyx", "Y": "zxy", "Z": "yxz", "G": "xyz"}
LANES = {"X": {"p": 512, "o": 384}, "Y": {"p": 512, "o": 256}, "Z": {"p": 512, "o": 384}, "G": {"g": 32}}
GROUPS = {8: ((0, 1), (1, 2), (3, 2), (5, 3)), 4: ((0, 1), (1, 2), (3, 1))}
RANK = {"g": (-1, -1, -1), "p": (0, 1, 3), "o": (1, 3, 7)}
RATE, LATENCY, ISSUE, BEGIN = 46.6e3, 2.2, 0.1, 4.0


def slot(n, step, way):
    return n - 1 if step == n // 2 else 2 * step - (way < 0 and step > 0)


def list_copies():
    copies, index = [], {}

    def go_round(prefix, axis, size, first, cut):
        n, made = RING[axis], []
        for step in range(1, n // 2 + 1):
            for way in (1, -1):
                halves = (0, 1) if way > 0 else (1, 0)
                for half in halves[:1] if step == n // 2 else halves if cut else (None,):
                    key = prefix + (step, way, half)
                    before = prefix + (step - 1, way, half)
                    if before not in index:
                        before = prefix + (step - 1, way, None)
                    needs = first if step == 1 else [before]
                    index[key] = len(copies)
                    copies.append((key, size / (1 if half is None else 2), [index[k] for k in needs]))
                    made.append(key)
        return made

    for name, (first, second, last) in ORDER.items():
        n = RING[first]
        for part, lanes in LANES[name].items():
            made = go_round((part, name, 0, (0, n)), first, lanes * 32, [], False)
            for group in GROUPS[n] if part == "p" else ((0, n),):
                needs = [k for k in made if group[0] <= slot(n, k[4], k[5]) < sum(group)]
                size = lanes * 32 * group[1]
                passed = go_round((part, name, 1, group), second, size, needs, False)
                go_round((part, name, 2, group), last, size * RING[second], passed, part == "o")
    return copies


def arrange(copies):
    come, free, order = {}, {}, []
    left = set(range(len(copies)))

    def rank(i):
        part, name, ring, group, step, way, half = copies[i][0]
        return (RANK[part][ring] - 0.2 * step, i)

    while left:
        best = None
        ready = {}
        for i in left:
            if all(n in come for n in copies[i][2]):
                key = copies[i][0]
                at = max([come[n] for n in copies[i][2]] + [BEGIN]) + ISSUE
                ready.setdefault((ORDER[key[1]][key[2]], key[5]), []).append((at, i))
        for link in sorted(ready):
            begin = max(free.get(link, 0.0), min(ready[link])[0])
            pick = min((i for at, i in ready[link] if at <= begin + 1e-9), key=rank)
            if best is None or (begin, pick) < best[:2]:
                best = (begin, pick, link)
        begin, pick, link = best
        free[link] = begin + copies[pick][1] / RATE
        come[pick] = free[link] + LATENCY
        left.remove(pick)
        order.append((begin, pick))
    return order, come


COPIES = list_copies()
SENT, COME = arrange(COPIES)
PART = {}
for number, (copy_key, _, _) in enumerate(COPIES):
    PART.setdefault((copy_key[1], copy_key[0]), []).append(number)
FAR = [(0, 0), (1, 1), (1, -1), (2, 1), (2, -1), (3, 1), (3, -1), (4, 1)]
LAST = {}
for number, (copy_key, _, _) in enumerate(COPIES):
    if copy_key[:3] == ("o", "Z", 2):
        LAST.setdefault((copy_key[4], 1 if copy_key[4] == 4 else copy_key[5]), []).append(number)


def dot(a, b):
    return lax.dot_general(a, b, (((1,), (0,)), ((), ())), preferred_element_type=jnp.float32)


def dot_t(a, b):
    return lax.dot_general(a, b, (((1,), (1,)), ((), ())), preferred_element_type=jnp.float32)


def kernel(
    hidden, gain, wq, wk, wv, wo, cos_in, sin_in, out,
    px, py, pz, ox, oy, oz, sg, xs, cos, sin, normed, q_all, k_lo, k_hi, v_lo, v_hi,
    score, prob, ctx, acc, mine, gone, come,
    stage, local, staged, away, here, sent, got, out_sent, out_got,
):
    f, r = lax.axis_index("fsdp"), lax.axis_index("rep")
    at = {"z": f // 4, "y": f % 4, "x": r // 2}
    core = r % 2
    other = 1 - core
    partner = (f, at["x"] * 2 + other)

    def neighbour(axis, way):
        n = RING[axis]
        place = dict(at)
        place[axis] = (at[axis] + way + n) % n
        return (place["z"] * 4 + place["y"], place["x"] * 2 + core)

    barrier = pltpu.get_barrier_semaphore()
    peers = [partner] + [neighbour(axis, way) for axis in "xyz" for way in (1, -1)]
    for peer in peers:
        pl.semaphore_signal(barrier, inc=1, device_id=peer, device_id_type=MESH)

    buffers = {"Xp": px, "Yp": py, "Zp": pz, "Xo": ox, "Yo": oy, "Zo": oz, "Gg": sg}
    rows = pl.ds(pl.multiple_of(core * 8, 8), 8)
    own_rows = pl.ds(pl.multiple_of(core * SEQ, SEQ), SEQ)
    other_rows = pl.ds(pl.multiple_of(other * SEQ, SEQ), SEQ)

    def shares(t):
        def cut(ref, width, start, count):
            return ref.at[:, pl.ds(pl.multiple_of(t * width + start, 128), count)]

        for name, lane, source in (
            ("Xp", 0, cut(wq, 1024, 0, 512)),
            ("Yp", 0, cut(wq, 1024, 512, 512)),
            ("Zp", 0, cut(wk, 256, 0, 256)),
            ("Zp", 256, cut(wv, 256, 0, 256)),
            ("Xo", 0, cut(wo, 1024, 0, 384)),
            ("Yo", 0, cut(wo, 1024, 384, 256)),
            ("Zo", 0, cut(wo, 1024, 640, 384)),
        ):
            _, b, c = (at[axis] for axis in ORDER[name[0]])
            yield source, buffers[name].at[c, b, 0, rows, pl.ds(lane, source.shape[1])]
        yield gain, sg.at[at["z"], at["y"], 0, core]
        yield hidden, xs.at[own_rows]

    starting = []
    for i, (source, target) in enumerate(shares(core)):
        starting.append(pltpu.make_async_copy(source, target, local.at[i]))
        starting[-1].start()
    widths = [source.shape[1] for source, _ in list(shares(other))[:7]]
    kept = [stage.at[:, pl.ds(sum(widths[:i]), width)] for i, width in enumerate(widths)]
    staging = []
    for i, (source, _) in enumerate(list(shares(other))[:7]):
        staging.append(pltpu.make_async_copy(source, kept[i], staged.at[i]))
        staging[-1].start()
    tables = [
        pltpu.make_async_copy(cos_in, cos, local.at[9]),
        pltpu.make_async_copy(sin_in, sin, local.at[10]),
    ]
    for copy in tables:
        copy.start()
    pl.semaphore_wait(barrier, len(peers))
    for i, (source, target) in enumerate(shares(other)):
        if i < 7:
            staging[i].wait()
            source = kept[i]
        copy = pltpu.make_async_remote_copy(
            src_ref=source, dst_ref=target, send_sem=away.at[i], recv_sem=here.at[i],
            device_id=partner, device_id_type=MESH,
        )
        copy.start()
        starting.append(copy)
    count = len(starting) // 2
    for copy in starting[: count - 1] + starting[count : 2 * count - 1]:
        copy.wait()

    def halves(n, half):
        return pl.ds(0, n) if half is None else pl.ds(half * (n // 2), n // 2)

    def lane_half(n, half):
        first = (n // 128 + 1) // 2 * 128
        return pl.ds(0, n) if half is None else pl.ds(0, first) if half == 0 else pl.ds(first, n - first)

    def transfer(i):
        part, name, ring, group, step, way, half = COPIES[i][0]
        a, b, c = (at[axis] for axis in ORDER[name])
        axis = ORDER[name][ring]
        n = RING[axis]
        buffer = buffers[name + part]
        lanes = LANES[name][part]
        block = (at[axis] - way * (step - 1) + n) % n
        source = target = None
        if ring == 0:
            tail = (halves(2, half),) if part == "g" else (slice(None), lane_half(lanes, half))
            source = buffer.at[(c, b, slot(n, step - 1, way)) + tail]
            target = buffer.at[(c, b, slot(n, step, way)) + tail]
        elif ring == 1:
            slots = pl.ds(*group)
            if part == "g":
                source = target = buffer.at[c, block, halves(group[1], half)]
            else:
                source = target = buffer.at[c, block, slots, :, lane_half(lanes, half)]
        else:
            slots = pl.ds(*group)
            source = target = buffer.at[block, halves(RING[ORDER[name][1]], half), slots]
        return pltpu.make_async_remote_copy(
            src_ref=source, dst_ref=target, send_sem=sent.at[i], recv_sem=got.at[i],
            device_id=neighbour(axis, way), device_id_type=MESH,
        )

    def waiting(i):
        part, name, ring, group, step, way, half = COPIES[i][0]
        buffer = buffers[name + part]
        lanes = LANES[name][part]
        if ring == 0:
            tail = (halves(2, half),) if part == "g" else (slice(None), lane_half(lanes, half))
            ref = buffer.at[(0, 0, 0) + tail]
        elif ring == 1 and part == "g":
            ref = buffer.at[0, 0, halves(group[1], half)]
        elif ring == 1:
            ref = buffer.at[0, 0, pl.ds(*group), :, lane_half(lanes, half)]
        else:
            ref = buffer.at[0, halves(RING[ORDER[name][1]], half), pl.ds(*group)]
        return pltpu.make_async_remote_copy(
            src_ref=ref, dst_ref=ref, send_sem=sent.at[i], recv_sem=got.at[i],
            device_id=partner, device_id_type=MESH,
        )

    arrived = set()

    def await_copy(i):
        if i not in arrived:
            arrived.add(i)
            waiting(i).wait_recv()

    def slots_of(axis):
        n = RING[axis]
        found = []
        for place in range(n):
            d = (place - at[axis] + n) % n
            found.append(jnp.where(d == 0, 0, jnp.where(d <= n // 2, 2 * d - 1, 2 * (n - d))))
        return found

    place_slots = {axis: slots_of(axis) for axis in "yz"}

    def norm(lo):
        chosen = pl.ds(lo, 128)
        x = xs[chosen].astype(jnp.float32)
        scale = lax.rsqrt(jnp.mean(x * x, axis=-1, keepdims=True) + NORM_EPS)
        for tile in range(16):
            z, y = tile // 2, tile % 2 * 2
            weight = sg[z, y, 0, 0]
            for k in range(1, 16):
                weight = weight + sg[z, y + k // 8, k // 2 % 4, k % 2]
            lanes = slice(tile * 128, tile * 128 + 128)
            normed[chosen, lanes] = (x[:, lanes] * scale * weight).astype(jnp.bfloat16)

    lane = lax.broadcasted_iota(jnp.int32, (SEQ, 128), 1)

    def rope(t):
        turned = jnp.where(lane % 64 < 32, pltpu.roll(t, 96, 1), pltpu.roll(t, 32, 1))
        return t * cos[...] + turned * sin[...]

    def features(name, z, lo, n):
        first, second, last = ORDER[name[0]]
        pieces = []
        for y in range(4):
            for x in range(4):
                place = {"x": x, "y": y, "z": z}
                pieces.append(
                    buffers[name][place[last], place[second], place_slots[first][place[first]], :, lo : lo + n]
                )
        return pieces

    def columns(name, lo, n):
        return jnp.concatenate([piece for z in range(8) for piece in features(name, z, lo, n)], axis=0)

    def project_q(name, lo, start):
        t = dot(normed[...], columns(name, lo, 256))
        for s in range(2):
            for half in range(2):
                piece = rope(t[s * SEQ : s * SEQ + SEQ, half * 128 : half * 128 + 128])
                q_all[s * SEQ : s * SEQ + SEQ, start + half * 128 : start + half * 128 + 128] = (
                    piece * HD**-0.5
                ).astype(jnp.bfloat16)

    def project_kv(lo, turn, low, high):
        t = dot(normed[...], columns("Zp", lo, 256))
        for s in range(2):
            for pair in range(2):
                piece = t[s * SEQ : s * SEQ + SEQ, pair * 128 : pair * 128 + 128]
                if turn:
                    piece = rope(piece)
                moved = pltpu.roll(piece, 64, 1)
                zero = jnp.zeros_like(piece)
                here_rows = slice(s * SEQ, s * SEQ + SEQ)
                for odd in range(2):
                    same, swapped = jnp.where(lane < 64, piece, zero), jnp.where(lane < 64, zero, moved)
                    if odd:
                        same, swapped = jnp.where(lane < 64, moved, zero), jnp.where(lane < 64, zero, piece)
                    low[2 * pair + odd, here_rows] = same.astype(jnp.bfloat16)
                    high[2 * pair + odd, here_rows] = swapped.astype(jnp.bfloat16)

    def attend(s, head):
        here_rows = slice(s * SEQ, s * SEQ + SEQ)
        keys = (k_lo[head, here_rows], k_hi[head, here_rows])
        values = jnp.concatenate([v_lo[head, here_rows], v_hi[head, here_rows]], axis=0)
        for pair in range(2):
            start = head * 256 + pair * 128
            for odd in range(2):
                score[4 * s + 2 * pair + odd] = dot_t(q_all[here_rows, start : start + 128], keys[odd])
        for unit in range(4):
            for block in range(4):
                n = 128 * (block // 2 + 1)
                chosen = slice(block * 64, block * 64 + 64)
                seen = lax.broadcasted_iota(jnp.int32, (64, 128), 1) <= (
                    lax.broadcasted_iota(jnp.int32, (64, 128), 0) + block % 2 * 64
                )
                t = jnp.where(seen, score[4 * s + unit, chosen, n - 128 : n], -1e30)
                if n > 128:
                    t = jnp.concatenate([score[4 * s + unit, chosen, :128], t], axis=1)
                expo = jnp.exp(t - jnp.max(t, axis=-1, keepdims=True))
                share = pl.reciprocal(jnp.sum(expo, axis=-1, keepdims=True), approx=False)
                prob[2 * s + unit // 2, chosen, unit % 2 * SEQ : unit % 2 * SEQ + n] = (expo * share).astype(jnp.bfloat16)
        for pair in range(2):
            start = head * 256 + pair * 128
            ctx[here_rows, start : start + 128] = dot(prob[2 * s + pair], values).astype(jnp.bfloat16)

    def attend_both(head):
        for s in range(2):
            attend(s, head)

    def mix_first(z):
        weights = jnp.concatenate(
            [
                jnp.concatenate(features("Xo", z, 0, 384), axis=0),
                jnp.concatenate(features("Yo", z, 0, 256), axis=0),
            ],
            axis=1,
        )
        acc[z] = dot_t(ctx[:, :640], weights)

    def chunk_of(k):
        step, way = FAR[k]
        return (at["z"] - way * step + 8) % 8

    def leaving(k):
        return pltpu.make_async_remote_copy(
            src_ref=gone.at[k], dst_ref=come.at[k], send_sem=out_sent.at[k], recv_sem=out_got.at[k],
            device_id=partner, device_id_type=MESH,
        )

    def mix_last(k):
        z = chunk_of(k)
        weights = jnp.concatenate(features("Zo", z, 0, 384), axis=0)
        gone[k] = acc[z, other_rows] + dot_t(ctx[other_rows, 640:], weights)
        mine[k] = acc[z, own_rows] + dot_t(ctx[own_rows, 640:], weights)
        leaving(k).start()

    works = []

    def work(parts, cost, run, *args, needs=()):
        needs = list(needs) + [i for part in parts for i in PART[part]]
        works.append((max(COME[i] for i in needs), cost * 0.6, needs, run, args))

    def prepare():
        starting[count - 1].wait()
        starting[2 * count - 1].wait()
        for copy in tables:
            copy.wait()
        for pair in range(4):
            for odd in range(2):
                prob[pair, :128, odd * SEQ + 128 : odd * SEQ + SEQ] = jnp.zeros((128, 128), jnp.bfloat16)

    work([("G", "g")], 0.0, prepare)
    for lo in range(0, 2 * SEQ, 128):
        work([("G", "g")], 0.2, norm, lo)
    work([("Z", "p")], 0.8, project_kv, 0, True, k_lo, k_hi)
    work([("Z", "p")], 0.8, project_kv, 256, False, v_lo, v_hi)
    for name, start in (("X", 0), ("Y", 512)):
        for lo in (0, 256):
            work([(name, "p")], 0.8, project_q, name + "p", lo, start + lo)
    works[5:] = sorted(works[5:], key=lambda w: w[0])
    for name, heads in (("X", (0, 1)), ("Y", (2, 3))):
        for head in heads:
            work([(name, "p"), ("Z", "p")], 1.7, attend_both, head)
    for z in range(8):
        work([("X", "o"), ("Y", "o")], 0.4, mix_first, z)
    for k in range(8):
        work([], 0.3, mix_last, k, needs=LAST[FAR[k]] if k else [i for i in PART["Z", "o"] if COPIES[i][0][2] < 2])

    now = 0.0
    sending = []

    def do_work():
        nonlocal now
        ready, cost, needs, run, args = works.pop(0)
        for i in needs:
            await_copy(i)
        run(*args)
        now = max(now, ready) + cost

    for begin, i in SENT:
        while works and max(works[0][0], now) + works[0][1] <= begin + 0.3:
            do_work()
        for j in COPIES[i][2]:
            await_copy(j)
        transfer(i).start()
        now = max(now, begin)
        sending.append((begin + COPIES[i][1] / RATE + 3.0, i))
        while sending[0][0] < begin:
            waiting(sending.pop(0)[1]).wait_send()
    while works:
        do_work()
    for i in range(len(COPIES)):
        await_copy(i)

    for k in range(8):
        lanes = pl.ds(pl.multiple_of(chunk_of(k) * 256, 256), 256)
        leaving(k).wait_recv()
        out[:, lanes] = (xs[own_rows, lanes].astype(jnp.float32) + (mine[k] + come[k])).astype(jnp.bfloat16)
    for k in range(8):
        leaving(k).wait_send()
    for _, i in sending:
        waiting(i).wait_send()


def rope_tables():
    position = np.arange(SEQ, dtype=np.float64)
    freq = ROPE_BASE ** (-(np.arange(HD // 2) * 2.0) / HD)
    angle = position[:, None] * freq[None, :]
    cos = np.tile(np.cos(angle), (1, 4))
    sin = np.tile(np.concatenate([-np.sin(angle), np.sin(angle)], axis=1), (1, 2))
    return cos.astype(np.float32), sin.astype(np.float32)


def body(hidden, gain, wq, wk, wv, w_out):
    cos, sin = rope_tables()
    device = lax.axis_index("fsdp") * 8 + lax.axis_index("rep")
    spread = jnp.tile(gain.astype(jnp.float32), 16)
    spread = jnp.where(jnp.arange(128) // 8 == device % 16, spread, 0.0)[None, :]
    vmem = pltpu.VMEM
    bf16, f32 = jnp.bfloat16, jnp.float32
    n = len(COPIES)
    dma = pltpu.SemaphoreType.DMA
    anywhere = pl.BlockSpec(memory_space=pltpu.HBM)
    inside = pl.BlockSpec(memory_space=pltpu.VMEM)
    return pl.pallas_call(
        kernel,
        out_shape=jax.ShapeDtypeStruct((SEQ, D), bf16),
        in_specs=[anywhere] * 8,
        out_specs=inside,
        scratch_shapes=[
            vmem((4, 4, 8, 16, 512), bf16),
            vmem((4, 4, 8, 16, 512), bf16),
            vmem((8, 4, 4, 16, 512), bf16),
            vmem((4, 4, 8, 16, 384), bf16),
            vmem((4, 4, 8, 16, 256), bf16),
            vmem((8, 4, 4, 16, 384), bf16),
            vmem((8, 4, 4, 2, 1, 128), f32),
            vmem((2 * SEQ, D), bf16),
            vmem((SEQ, 128), f32),
            vmem((SEQ, 128), f32),
            vmem((2 * SEQ, D), bf16),
            vmem((2 * SEQ, 1024), bf16),
            vmem((4, 2 * SEQ, 128), bf16),
            vmem((4, 2 * SEQ, 128), bf16),
            vmem((4, 2 * SEQ, 128), bf16),
            vmem((4, 2 * SEQ, 128), bf16),
            vmem((8, SEQ, SEQ), f32),
            vmem((4, SEQ, 2 * SEQ), bf16),
            vmem((2 * SEQ, 1024), bf16),
            vmem((8, 2 * SEQ, 256), f32),
            vmem((8, SEQ, 256), f32),
            vmem((8, SEQ, 256), f32),
            vmem((8, SEQ, 256), f32),
            vmem((8, 2560), bf16),
            dma((11,)), dma((7,)), dma((9,)), dma((9,)), dma((n,)), dma((n,)), dma((8,)), dma((8,)),
        ],
        compiler_params=pltpu.CompilerParams(
            collective_id=0, has_side_effects=True, vmem_limit_bytes=40 * 2**20
        ),
        name="attention_block",
    )(*(pltpu.with_memory_space_constraint(a, pltpu.HBM) for a in (hidden, spread, wq, wk, wv, w_out.T, cos, sin)))


def solution(mesh):
    rows = P(("fsdp", "rep"), None)
    placed = (rows, P(("fsdp", "rep")), rows, rows, rows, P(None, ("fsdp", "rep")))
    return jax.shard_map(body, mesh=mesh, in_specs=placed, out_specs=rows, check_vma=False)
```

```python
import jax
import jax.numpy as jnp
import numpy as np
from jax import lax
from jax.experimental import pallas as pl
from jax.experimental.pallas import tpu as pltpu
from jax.sharding import PartitionSpec as P

HD = 64
SEQ = 256
D = 2048
ROPE_BASE = 500000.0
NORM_EPS = 1e-05
MESH = pl.DeviceIdType.MESH

RING = {"x": 4, "y": 4, "z": 8}
ORDER = {"X": "zyx", "Y": "zxy", "Z": "yxz", "G": "xyz"}
LANES = {"X": {"p": 512, "o": 384}, "Y": {"p": 512, "o": 256}, "Z": {"p": 512, "o": 384}, "G": {"g": 32}}
GROUPS = {8: ((0, 1), (1, 2), (3, 2), (5, 3)), 4: ((0, 1), (1, 2), (3, 1))}
RANK = {"g": (-1, -1, -1), "p": (0, 1, 3), "o": (1, 3, 7)}
RATE, LATENCY, ISSUE, BEGIN = 46.6e3, 2.3, 0.1, 5.5


def slot(n, step, way):
    return n - 1 if step == n // 2 else 2 * step - (way < 0 and step > 0)


def list_copies():
    copies, index = [], {}

    def go_round(prefix, axis, size, first, cut):
        n, made = RING[axis], []
        for step in range(1, n // 2 + 1):
            for way in (1, -1):
                halves = (0, 1) if way > 0 else (1, 0)
                for half in halves[:1] if step == n // 2 else halves if cut else (None,):
                    key = prefix + (step, way, half)
                    before = prefix + (step - 1, way, half)
                    if before not in index:
                        before = prefix + (step - 1, way, None)
                    needs = first if step == 1 else [before]
                    index[key] = len(copies)
                    copies.append((key, size / (1 if half is None else 2), [index[k] for k in needs]))
                    made.append(key)
        return made

    for name, (first, second, last) in ORDER.items():
        n = RING[first]
        for part, lanes in LANES[name].items():
            made = go_round((part, name, 0, (0, n)), first, lanes * 32, [], False)
            for group in GROUPS[n] if part == "p" else ((0, n),):
                needs = [k for k in made if group[0] <= slot(n, k[4], k[5]) < sum(group)]
                size = lanes * 32 * group[1]
                passed = go_round((part, name, 1, group), second, size, needs, False)
                go_round((part, name, 2, group), last, size * RING[second], passed, part == "o")
    return copies


def arrange(copies):
    come, free, order = {}, {}, []
    left = set(range(len(copies)))

    def rank(i):
        part, name, ring, group, step, way, half = copies[i][0]
        return (RANK[part][ring] - 0.2 * step, i)

    while left:
        best = None
        ready = {}
        for i in left:
            if all(n in come for n in copies[i][2]):
                key = copies[i][0]
                at = max([come[n] for n in copies[i][2]] + [BEGIN]) + ISSUE
                ready.setdefault((ORDER[key[1]][key[2]], key[5]), []).append((at, i))
        for link in sorted(ready):
            begin = max(free.get(link, 0.0), min(ready[link])[0])
            pick = min((i for at, i in ready[link] if at <= begin + 1e-9), key=rank)
            if best is None or (begin, pick) < best[:2]:
                best = (begin, pick, link)
        begin, pick, link = best
        free[link] = begin + copies[pick][1] / RATE
        come[pick] = free[link] + LATENCY
        left.remove(pick)
        order.append((begin, pick))
    return order, come


COPIES = list_copies()
SENT, COME = arrange(COPIES)
PART = {}
for number, (copy_key, _, _) in enumerate(COPIES):
    PART.setdefault((copy_key[1], copy_key[0]), []).append(number)
FAR = [(0, 0), (1, 1), (1, -1), (2, 1), (2, -1), (3, 1), (3, -1), (4, 1)]
LAST = {}
for number, (copy_key, _, _) in enumerate(COPIES):
    if copy_key[:3] == ("o", "Z", 2):
        LAST.setdefault((copy_key[4], 1 if copy_key[4] == 4 else copy_key[5]), []).append(number)


def dot(a, b):
    return lax.dot_general(a, b, (((1,), (0,)), ((), ())), preferred_element_type=jnp.float32)


def dot_t(a, b):
    return lax.dot_general(a, b, (((1,), (1,)), ((), ())), preferred_element_type=jnp.float32)


def kernel(
    hidden, gain, wq, wk, wv, wo, cos_in, sin_in, out,
    px, py, pz, ox, oy, oz, sg, xs, cos, sin, normed, q_all, k_lo, k_hi, v_lo, v_hi,
    score, prob, ctx, acc, mine, gone, come,
    stage, few, local, staged, away, here, sent, got, out_sent, out_got,
):
    f, r = lax.axis_index("fsdp"), lax.axis_index("rep")
    at = {"z": f // 4, "y": f % 4, "x": r // 2}
    core = r % 2
    other = 1 - core
    partner = (f, at["x"] * 2 + other)

    def neighbour(axis, way):
        n = RING[axis]
        place = dict(at)
        place[axis] = (at[axis] + way + n) % n
        return (place["z"] * 4 + place["y"], place["x"] * 2 + core)

    barrier = pltpu.get_barrier_semaphore()
    peers = [partner] + [neighbour(axis, way) for axis in "xyz" for way in (1, -1)]
    for peer in peers:
        pl.semaphore_signal(barrier, inc=1, device_id=peer, device_id_type=MESH)

    buffers = {"Xp": px, "Yp": py, "Zp": pz, "Xo": ox, "Yo": oy, "Zo": oz, "Gg": sg}
    rows = pl.ds(pl.multiple_of(core * 8, 8), 8)
    own_rows = pl.ds(pl.multiple_of(core * SEQ, SEQ), SEQ)
    other_rows = pl.ds(pl.multiple_of(other * SEQ, SEQ), SEQ)

    def shares(t):
        def cut(ref, width, start, count):
            return ref.at[:, pl.ds(pl.multiple_of(t * width + start, 128), count)]

        for name, lane, source in (
            ("Xp", 0, cut(wq, 1024, 0, 512)),
            ("Yp", 0, cut(wq, 1024, 512, 512)),
            ("Zp", 0, cut(wk, 256, 0, 256)),
            ("Zp", 256, cut(wv, 256, 0, 256)),
            ("Xo", 0, cut(wo, 1024, 0, 384)),
            ("Yo", 0, cut(wo, 1024, 384, 256)),
            ("Zo", 0, cut(wo, 1024, 640, 384)),
        ):
            _, b, c = (at[axis] for axis in ORDER[name[0]])
            yield source, buffers[name].at[c, b, 0, rows, pl.ds(lane, source.shape[1])]
        if t is other:
            yield own_gain, own_gain
        yield hidden, xs.at[own_rows]

    own_gain = sg.at[at["z"], at["y"], 0, core]
    taking = pltpu.make_async_copy(gain, few, staged.at[7])
    taking.start()
    starting = []
    for i, (source, target) in enumerate(shares(core)):
        starting.append(pltpu.make_async_copy(source, target, local.at[i]))
        starting[-1].start()
    widths = [source.shape[1] for source, _ in list(shares(other))[:7]]
    kept = [stage.at[:, pl.ds(sum(widths[:i]), width)] for i, width in enumerate(widths)]
    staging = []
    for i, (source, _) in enumerate(list(shares(other))[:7]):
        staging.append(pltpu.make_async_copy(source, kept[i], staged.at[i]))
        staging[-1].start()
    tables = [
        pltpu.make_async_copy(cos_in, cos, local.at[9]),
        pltpu.make_async_copy(sin_in, sin, local.at[10]),
    ]
    for copy in tables:
        copy.start()
    taking.wait()
    spread = jnp.concatenate([few[...].astype(jnp.float32).reshape(1, 8)] * 16, axis=1)
    place = lax.broadcasted_iota(jnp.int32, (1, 128), 1) // 8
    sg[at["z"], at["y"], 0, core] = jnp.where(place == f % 2 * 8 + r, spread, 0.0)
    pl.semaphore_wait(barrier, len(peers))
    for i, (source, target) in enumerate(shares(other)):
        if i < 7:
            staging[i].wait()
            source = kept[i]
        copy = pltpu.make_async_remote_copy(
            src_ref=source, dst_ref=target, send_sem=away.at[i], recv_sem=here.at[i],
            device_id=partner, device_id_type=MESH,
        )
        copy.start()
        starting.append(copy)
    for copy in starting[:7] + starting[8:16]:
        copy.wait()

    def halves(n, half):
        return pl.ds(0, n) if half is None else pl.ds(half * (n // 2), n // 2)

    def lane_half(n, half):
        first = (n // 128 + 1) // 2 * 128
        return pl.ds(0, n) if half is None else pl.ds(0, first) if half == 0 else pl.ds(first, n - first)

    def transfer(i):
        part, name, ring, group, step, way, half = COPIES[i][0]
        a, b, c = (at[axis] for axis in ORDER[name])
        axis = ORDER[name][ring]
        n = RING[axis]
        buffer = buffers[name + part]
        lanes = LANES[name][part]
        block = (at[axis] - way * (step - 1) + n) % n
        source = target = None
        if ring == 0:
            tail = (halves(2, half),) if part == "g" else (slice(None), lane_half(lanes, half))
            source = buffer.at[(c, b, slot(n, step - 1, way)) + tail]
            target = buffer.at[(c, b, slot(n, step, way)) + tail]
        elif ring == 1:
            slots = pl.ds(*group)
            if part == "g":
                source = target = buffer.at[c, block, halves(group[1], half)]
            else:
                source = target = buffer.at[c, block, slots, :, lane_half(lanes, half)]
        else:
            slots = pl.ds(*group)
            source = target = buffer.at[block, halves(RING[ORDER[name][1]], half), slots]
        return pltpu.make_async_remote_copy(
            src_ref=source, dst_ref=target, send_sem=sent.at[i], recv_sem=got.at[i],
            device_id=neighbour(axis, way), device_id_type=MESH,
        )

    def waiting(i):
        part, name, ring, group, step, way, half = COPIES[i][0]
        buffer = buffers[name + part]
        lanes = LANES[name][part]
        if ring == 0:
            tail = (halves(2, half),) if part == "g" else (slice(None), lane_half(lanes, half))
            ref = buffer.at[(0, 0, 0) + tail]
        elif ring == 1 and part == "g":
            ref = buffer.at[0, 0, halves(group[1], half)]
        elif ring == 1:
            ref = buffer.at[0, 0, pl.ds(*group), :, lane_half(lanes, half)]
        else:
            ref = buffer.at[0, halves(RING[ORDER[name][1]], half), pl.ds(*group)]
        return pltpu.make_async_remote_copy(
            src_ref=ref, dst_ref=ref, send_sem=sent.at[i], recv_sem=got.at[i],
            device_id=partner, device_id_type=MESH,
        )

    arrived = set()

    def await_copy(i):
        if i not in arrived:
            arrived.add(i)
            waiting(i).wait_recv()

    def slots_of(axis):
        n = RING[axis]
        found = []
        for place in range(n):
            d = (place - at[axis] + n) % n
            found.append(jnp.where(d == 0, 0, jnp.where(d <= n // 2, 2 * d - 1, 2 * (n - d))))
        return found

    place_slots = {axis: slots_of(axis) for axis in "yz"}

    def norm(lo):
        chosen = pl.ds(lo, 128)
        x = xs[chosen].astype(jnp.float32)
        scale = lax.rsqrt(jnp.mean(x * x, axis=-1, keepdims=True) + NORM_EPS)
        for tile in range(16):
            z, y = tile // 2, tile % 2 * 2
            weight = sg[z, y, 0, 0]
            for k in range(1, 16):
                weight = weight + sg[z, y + k // 8, k // 2 % 4, k % 2]
            lanes = slice(tile * 128, tile * 128 + 128)
            normed[chosen, lanes] = (x[:, lanes] * scale * weight).astype(jnp.bfloat16)

    lane = lax.broadcasted_iota(jnp.int32, (SEQ, 128), 1)

    def rope(t):
        turned = jnp.where(lane % 64 < 32, pltpu.roll(t, 96, 1), pltpu.roll(t, 32, 1))
        return t * cos[...] + turned * sin[...]

    def features(name, z, lo, n):
        first, second, last = ORDER[name[0]]
        pieces = []
        for y in range(4):
            for x in range(4):
                place = {"x": x, "y": y, "z": z}
                pieces.append(
                    buffers[name][place[last], place[second], place_slots[first][place[first]], :, lo : lo + n]
                )
        return pieces

    def columns(name, lo, n):
        return jnp.concatenate([piece for z in range(8) for piece in features(name, z, lo, n)], axis=0)

    def project_q(name, lo, start):
        t = dot(normed[...], columns(name, lo, 256))
        for s in range(2):
            for half in range(2):
                piece = rope(t[s * SEQ : s * SEQ + SEQ, half * 128 : half * 128 + 128])
                q_all[s * SEQ : s * SEQ + SEQ, start + half * 128 : start + half * 128 + 128] = (
                    piece * HD**-0.5
                ).astype(jnp.bfloat16)

    def project_two(name, start):
        project_q(name, 0, start)
        project_q(name, 256, start + 256)

    def project_kv(lo, turn, low, high):
        t = dot(normed[...], columns("Zp", lo, 256))
        for s in range(2):
            for pair in range(2):
                piece = t[s * SEQ : s * SEQ + SEQ, pair * 128 : pair * 128 + 128]
                if turn:
                    piece = rope(piece)
                moved = pltpu.roll(piece, 64, 1)
                zero = jnp.zeros_like(piece)
                here_rows = slice(s * SEQ, s * SEQ + SEQ)
                for odd in range(2):
                    same, swapped = jnp.where(lane < 64, piece, zero), jnp.where(lane < 64, zero, moved)
                    if odd:
                        same, swapped = jnp.where(lane < 64, moved, zero), jnp.where(lane < 64, zero, piece)
                    low[2 * pair + odd, here_rows] = same.astype(jnp.bfloat16)
                    high[2 * pair + odd, here_rows] = swapped.astype(jnp.bfloat16)

    def attend(s, head):
        here_rows = slice(s * SEQ, s * SEQ + SEQ)
        keys = (k_lo[head, here_rows], k_hi[head, here_rows])
        values = jnp.concatenate([v_lo[head, here_rows], v_hi[head, here_rows]], axis=0)
        for pair in range(2):
            start = head * 256 + pair * 128
            for odd in range(2):
                score[4 * s + 2 * pair + odd] = dot_t(q_all[here_rows, start : start + 128], keys[odd])
        for unit in range(4):
            for block in range(4):
                n = 128 * (block // 2 + 1)
                chosen = slice(block * 64, block * 64 + 64)
                seen = lax.broadcasted_iota(jnp.int32, (64, 128), 1) <= (
                    lax.broadcasted_iota(jnp.int32, (64, 128), 0) + block % 2 * 64
                )
                t = jnp.where(seen, score[4 * s + unit, chosen, n - 128 : n], -1e30)
                if n > 128:
                    t = jnp.concatenate([score[4 * s + unit, chosen, :128], t], axis=1)
                expo = jnp.exp(t - jnp.max(t, axis=-1, keepdims=True))
                share = pl.reciprocal(jnp.sum(expo, axis=-1, keepdims=True), approx=False)
                prob[2 * s + unit // 2, chosen, unit % 2 * SEQ : unit % 2 * SEQ + n] = (expo * share).astype(jnp.bfloat16)
        for pair in range(2):
            start = head * 256 + pair * 128
            ctx[here_rows, start : start + 128] = dot(prob[2 * s + pair], values).astype(jnp.bfloat16)

    def attend_both(head):
        for s in range(2):
            attend(s, head)

    def mix_first(z):
        weights = jnp.concatenate(
            [
                jnp.concatenate(features("Xo", z, 0, 384), axis=0),
                jnp.concatenate(features("Yo", z, 0, 256), axis=0),
            ],
            axis=1,
        )
        acc[z] = dot_t(ctx[:, :640], weights)

    def mix_two(z):
        mix_first(z)
        mix_first(z + 1)

    def chunk_of(k):
        step, way = FAR[k]
        return (at["z"] - way * step + 8) % 8

    def leaving(k):
        return pltpu.make_async_remote_copy(
            src_ref=gone.at[k], dst_ref=come.at[k], send_sem=out_sent.at[k], recv_sem=out_got.at[k],
            device_id=partner, device_id_type=MESH,
        )

    def mix_last(k):
        z = chunk_of(k)
        weights = jnp.concatenate(features("Zo", z, 0, 384), axis=0)
        gone[k] = acc[z, other_rows] + dot_t(ctx[other_rows, 640:], weights)
        mine[k] = acc[z, own_rows] + dot_t(ctx[own_rows, 640:], weights)
        leaving(k).start()

    works = []

    def work(parts, cost, run, *args, needs=()):
        needs = list(needs) + [i for part in parts for i in PART[part]]
        works.append((max(COME[i] for i in needs), cost * 0.7, needs, run, args))

    def prepare():
        starting[7].wait()
        starting[16].wait()
        for copy in tables:
            copy.wait()
        for pair in range(4):
            for odd in range(2):
                prob[pair, :128, odd * SEQ + 128 : odd * SEQ + SEQ] = jnp.zeros((128, 128), jnp.bfloat16)

    work([("G", "g")], 0.0, prepare)
    for lo in range(0, 2 * SEQ, 128):
        work([("G", "g")], 0.2, norm, lo)
    work([("Z", "p")], 0.8, project_kv, 0, True, k_lo, k_hi)
    work([("Z", "p")], 0.8, project_kv, 256, False, v_lo, v_hi)
    for name, start in (("X", 0), ("Y", 512)):
        work([(name, "p")], 1.4, project_two, name + "p", start)
    works[5:] = sorted(works[5:], key=lambda w: w[0])
    for name, heads in (("X", (0, 1)), ("Y", (2, 3))):
        for head in heads:
            work([(name, "p"), ("Z", "p")], 1.7, attend_both, head)
    for z in range(0, 8, 2):
        work([("X", "o"), ("Y", "o")], 0.9, mix_two, z)
    for k in range(8):
        work([], 0.3, mix_last, k, needs=LAST[FAR[k]] if k else [i for i in PART["Z", "o"] if COPIES[i][0][2] < 2])

    now = 0.0
    sending = []

    def do_work():
        nonlocal now
        ready, cost, needs, run, args = works.pop(0)
        for i in needs:
            await_copy(i)
        run(*args)
        now = max(now, ready) + cost

    for begin, i in SENT:
        while works and max(works[0][0], now) + works[0][1] <= begin + 0.3:
            do_work()
        for j in COPIES[i][2]:
            await_copy(j)
        transfer(i).start()
        now = max(now, begin)
        sending.append((begin + COPIES[i][1] / RATE + 3.0, i))
        while sending[0][0] < begin:
            waiting(sending.pop(0)[1]).wait_send()
    while works:
        do_work()
    for i in range(len(COPIES)):
        await_copy(i)

    for k in range(8):
        lanes = pl.ds(pl.multiple_of(chunk_of(k) * 256, 256), 256)
        leaving(k).wait_recv()
        out[:, lanes] = (xs[own_rows, lanes].astype(jnp.float32) + (mine[k] + come[k])).astype(jnp.bfloat16)
    for k in range(8):
        leaving(k).wait_send()
    for _, i in sending:
        waiting(i).wait_send()


def rope_tables():
    position = np.arange(SEQ, dtype=np.float64)
    freq = ROPE_BASE ** (-(np.arange(HD // 2) * 2.0) / HD)
    angle = position[:, None] * freq[None, :]
    cos = np.tile(np.cos(angle), (1, 4))
    sin = np.tile(np.concatenate([-np.sin(angle), np.sin(angle)], axis=1), (1, 2))
    return cos.astype(np.float32), sin.astype(np.float32)


def body(hidden, gain, wq, wk, wv, w_out):
    cos, sin = rope_tables()
    vmem = pltpu.VMEM
    bf16, f32 = jnp.bfloat16, jnp.float32
    n = len(COPIES)
    dma = pltpu.SemaphoreType.DMA
    anywhere = pl.BlockSpec(memory_space=pltpu.HBM)
    inside = pl.BlockSpec(memory_space=pltpu.VMEM)
    return pl.pallas_call(
        kernel,
        out_shape=jax.ShapeDtypeStruct((SEQ, D), bf16),
        in_specs=[anywhere] * 8,
        out_specs=inside,
        scratch_shapes=[
            vmem((4, 4, 8, 16, 512), bf16),
            vmem((4, 4, 8, 16, 512), bf16),
            vmem((8, 4, 4, 16, 512), bf16),
            vmem((4, 4, 8, 16, 384), bf16),
            vmem((4, 4, 8, 16, 256), bf16),
            vmem((8, 4, 4, 16, 384), bf16),
            vmem((8, 4, 4, 2, 1, 128), f32),
            vmem((2 * SEQ, D), bf16),
            vmem((SEQ, 128), f32),
            vmem((SEQ, 128), f32),
            vmem((2 * SEQ, D), bf16),
            vmem((2 * SEQ, 1024), bf16),
            vmem((4, 2 * SEQ, 128), bf16),
            vmem((4, 2 * SEQ, 128), bf16),
            vmem((4, 2 * SEQ, 128), bf16),
            vmem((4, 2 * SEQ, 128), bf16),
            vmem((8, SEQ, SEQ), f32),
            vmem((4, SEQ, 2 * SEQ), bf16),
            vmem((2 * SEQ, 1024), bf16),
            vmem((8, 2 * SEQ, 256), f32),
            vmem((8, SEQ, 256), f32),
            vmem((8, SEQ, 256), f32),
            vmem((8, SEQ, 256), f32),
            vmem((8, 2560), bf16),
            vmem((8,), bf16),
            dma((11,)), dma((8,)), dma((9,)), dma((9,)), dma((n,)), dma((n,)), dma((8,)), dma((8,)),
        ],
        compiler_params=pltpu.CompilerParams(
            collective_id=0, has_side_effects=True, vmem_limit_bytes=40 * 2**20
        ),
        name="attention_block",
    )(*(pltpu.with_memory_space_constraint(a, pltpu.HBM) for a in (hidden, gain, wq, wk, wv, w_out.T, cos, sin)))


def solution(mesh):
    rows = P(("fsdp", "rep"), None)
    placed = (rows, P(("fsdp", "rep")), rows, rows, rows, P(None, ("fsdp", "rep")))
    return jax.shard_map(body, mesh=mesh, in_specs=placed, out_specs=rows, check_vma=False)
```

```python
import jax
import jax.numpy as jnp
import numpy as np
from jax import lax
from jax.experimental import pallas as pl
from jax.experimental.pallas import tpu as pltpu
from jax.sharding import PartitionSpec as P

HD = 64
SEQ = 256
D = 2048
ROPE_BASE = 500000.0
NORM_EPS = 1e-05
MESH = pl.DeviceIdType.MESH

RING = {"x": 4, "y": 4, "z": 8}
ORDER = {"X": "zyx", "Y": "zxy", "Z": "yxz", "G": "xyz"}
LANES = {"X": {"p": 512, "o": 384}, "Y": {"p": 512, "o": 256}, "Z": {"p": 512, "o": 384}, "G": {"g": 32}}
GROUPS = {8: ((0, 1), (1, 2), (3, 2), (5, 3)), 4: ((0, 1), (1, 2), (3, 1))}
RANK = {"g": (-1, -1, -1), "p": (0, 1, 3), "o": (1, 3, 7)}
RATE, LATENCY, ISSUE, BEGIN = 46.6e3, 2.3, 0.1, 5.5


def slot(n, step, way):
    return n - 1 if step == n // 2 else 2 * step - (way < 0 and step > 0)


def list_copies():
    copies, index = [], {}

    def go_round(prefix, axis, size, first, cut):
        n, made = RING[axis], []
        for step in range(1, n // 2 + 1):
            for way in (1, -1):
                halves = (0, 1) if way > 0 else (1, 0)
                for half in halves[:1] if step == n // 2 else halves if cut else (None,):
                    key = prefix + (step, way, half)
                    before = prefix + (step - 1, way, half)
                    if before not in index:
                        before = prefix + (step - 1, way, None)
                    needs = first if step == 1 else [before]
                    index[key] = len(copies)
                    copies.append((key, size / (1 if half is None else 2), [index[k] for k in needs]))
                    made.append(key)
        return made

    for name, (first, second, last) in ORDER.items():
        n = RING[first]
        for part, lanes in LANES[name].items():
            made = go_round((part, name, 0, (0, n)), first, lanes * 32, [], False)
            for group in GROUPS[n] if part == "p" else ((0, n),):
                needs = [k for k in made if group[0] <= slot(n, k[4], k[5]) < sum(group)]
                size = lanes * 32 * group[1]
                passed = go_round((part, name, 1, group), second, size, needs, False)
                go_round((part, name, 2, group), last, size * RING[second], passed, part == "o")
    return copies


def arrange(copies):
    come, free, order = {}, {}, []
    left = set(range(len(copies)))

    def rank(i):
        part, name, ring, group, step, way, half = copies[i][0]
        return (RANK[part][ring] - 0.2 * step, i)

    while left:
        best = None
        ready = {}
        for i in left:
            if all(n in come for n in copies[i][2]):
                key = copies[i][0]
                at = max([come[n] for n in copies[i][2]] + [BEGIN]) + ISSUE
                ready.setdefault((ORDER[key[1]][key[2]], key[5]), []).append((at, i))
        for link in sorted(ready):
            begin = max(free.get(link, 0.0), min(ready[link])[0])
            pick = min((i for at, i in ready[link] if at <= begin + 1e-9), key=rank)
            if best is None or (begin, pick) < best[:2]:
                best = (begin, pick, link)
        begin, pick, link = best
        free[link] = begin + copies[pick][1] / RATE
        come[pick] = free[link] + LATENCY
        left.remove(pick)
        order.append((begin, pick))
    return order, come


COPIES = list_copies()
SENT, COME = arrange(COPIES)
PART = {}
for number, (copy_key, _, _) in enumerate(COPIES):
    PART.setdefault((copy_key[1], copy_key[0]), []).append(number)
FAR = [(0, 0), (1, 1), (1, -1), (2, 1), (2, -1), (3, 1), (3, -1), (4, 1)]
LAST = {}
for number, (copy_key, _, _) in enumerate(COPIES):
    if copy_key[:3] == ("o", "Z", 2):
        LAST.setdefault((copy_key[4], 1 if copy_key[4] == 4 else copy_key[5]), []).append(number)


def dot(a, b):
    return lax.dot_general(a, b, (((1,), (0,)), ((), ())), preferred_element_type=jnp.float32)


def dot_t(a, b):
    return lax.dot_general(a, b, (((1,), (1,)), ((), ())), preferred_element_type=jnp.float32)


def kernel(
    hidden, gain, wq, wk, wv, wo, cos_in, sin_in, out,
    px, py, pz, ox, oy, oz, sg, xs, cos, sin, normed, q_all, k_lo, k_hi, v_lo, v_hi,
    score, prob, ctx, acc, mine, gone, come,
    stage, few, local, staged, away, here, sent, got, out_sent, out_got,
):
    f, r = lax.axis_index("fsdp"), lax.axis_index("rep")
    at = {"z": f // 4, "y": f % 4, "x": r // 2}
    core = r % 2
    other = 1 - core
    partner = (f, at["x"] * 2 + other)

    def neighbour(axis, way):
        n = RING[axis]
        place = dict(at)
        place[axis] = (at[axis] + way + n) % n
        return (place["z"] * 4 + place["y"], place["x"] * 2 + core)

    barrier = pltpu.get_barrier_semaphore()
    peers = [partner] + [neighbour(axis, way) for axis in "xyz" for way in (1, -1)]
    for peer in peers:
        pl.semaphore_signal(barrier, inc=1, device_id=peer, device_id_type=MESH)

    buffers = {"Xp": px, "Yp": py, "Zp": pz, "Xo": ox, "Yo": oy, "Zo": oz, "Gg": sg}
    rows = pl.ds(pl.multiple_of(core * 8, 8), 8)
    own_rows = pl.ds(pl.multiple_of(core * SEQ, SEQ), SEQ)
    other_rows = pl.ds(pl.multiple_of(other * SEQ, SEQ), SEQ)

    def shares(t):
        def cut(ref, width, start, count):
            return ref.at[:, pl.ds(pl.multiple_of(t * width + start, 128), count)]

        for name, lane, source in (
            ("Xp", 0, cut(wq, 1024, 0, 512)),
            ("Yp", 0, cut(wq, 1024, 512, 512)),
            ("Zp", 0, cut(wk, 256, 0, 256)),
            ("Zp", 256, cut(wv, 256, 0, 256)),
            ("Xo", 0, cut(wo, 1024, 0, 384)),
            ("Yo", 0, cut(wo, 1024, 384, 256)),
            ("Zo", 0, cut(wo, 1024, 640, 384)),
        ):
            _, b, c = (at[axis] for axis in ORDER[name[0]])
            yield source, buffers[name].at[c, b, 0, rows, pl.ds(lane, source.shape[1])]
        if t is other:
            yield own_gain, own_gain
        yield hidden, xs.at[own_rows]

    own_gain = sg.at[at["z"], at["y"], 0, core]
    taking = pltpu.make_async_copy(gain, few, staged.at[7])
    taking.start()
    widths = [source.shape[1] for source, _ in list(shares(other))[:7]]
    kept = [stage.at[:, pl.ds(sum(widths[:i]), width)] for i, width in enumerate(widths)]
    staging = []
    for i, (source, _) in enumerate(list(shares(other))[:7]):
        staging.append(pltpu.make_async_copy(source, kept[i], staged.at[i]))
        staging[-1].start()
    starting = []
    for i, (source, target) in enumerate(shares(core)):
        starting.append(pltpu.make_async_copy(source, target, local.at[i]))
        starting[-1].start()
    tables = [
        pltpu.make_async_copy(cos_in, cos, local.at[9]),
        pltpu.make_async_copy(sin_in, sin, local.at[10]),
    ]
    for copy in tables:
        copy.start()
    taking.wait()
    spread = jnp.concatenate([few[...].astype(jnp.float32).reshape(1, 8)] * 16, axis=1)
    place = lax.broadcasted_iota(jnp.int32, (1, 128), 1) // 8
    sg[at["z"], at["y"], 0, core] = jnp.where(place == f % 2 * 8 + r, spread, 0.0)
    pl.semaphore_wait(barrier, len(peers))
    for i, (source, target) in enumerate(shares(other)):
        if i < 7:
            staging[i].wait()
            source = kept[i]
        copy = pltpu.make_async_remote_copy(
            src_ref=source, dst_ref=target, send_sem=away.at[i], recv_sem=here.at[i],
            device_id=partner, device_id_type=MESH,
        )
        copy.start()
        starting.append(copy)
    for copy in starting[:7] + starting[8:16]:
        copy.wait()

    def halves(n, half):
        return pl.ds(0, n) if half is None else pl.ds(half * (n // 2), n // 2)

    def lane_half(n, half):
        first = (n // 128 + 1) // 2 * 128
        return pl.ds(0, n) if half is None else pl.ds(0, first) if half == 0 else pl.ds(first, n - first)

    def transfer(i):
        part, name, ring, group, step, way, half = COPIES[i][0]
        a, b, c = (at[axis] for axis in ORDER[name])
        axis = ORDER[name][ring]
        n = RING[axis]
        buffer = buffers[name + part]
        lanes = LANES[name][part]
        block = (at[axis] - way * (step - 1) + n) % n
        source = target = None
        if ring == 0:
            tail = (halves(2, half),) if part == "g" else (slice(None), lane_half(lanes, half))
            source = buffer.at[(c, b, slot(n, step - 1, way)) + tail]
            target = buffer.at[(c, b, slot(n, step, way)) + tail]
        elif ring == 1:
            slots = pl.ds(*group)
            if part == "g":
                source = target = buffer.at[c, block, halves(group[1], half)]
            else:
                source = target = buffer.at[c, block, slots, :, lane_half(lanes, half)]
        else:
            slots = pl.ds(*group)
            source = target = buffer.at[block, halves(RING[ORDER[name][1]], half), slots]
        return pltpu.make_async_remote_copy(
            src_ref=source, dst_ref=target, send_sem=sent.at[i], recv_sem=got.at[i],
            device_id=neighbour(axis, way), device_id_type=MESH,
        )

    def waiting(i):
        part, name, ring, group, step, way, half = COPIES[i][0]
        buffer = buffers[name + part]
        lanes = LANES[name][part]
        if ring == 0:
            tail = (halves(2, half),) if part == "g" else (slice(None), lane_half(lanes, half))
            ref = buffer.at[(0, 0, 0) + tail]
        elif ring == 1 and part == "g":
            ref = buffer.at[0, 0, halves(group[1], half)]
        elif ring == 1:
            ref = buffer.at[0, 0, pl.ds(*group), :, lane_half(lanes, half)]
        else:
            ref = buffer.at[0, halves(RING[ORDER[name][1]], half), pl.ds(*group)]
        return pltpu.make_async_remote_copy(
            src_ref=ref, dst_ref=ref, send_sem=sent.at[i], recv_sem=got.at[i],
            device_id=partner, device_id_type=MESH,
        )

    arrived = set()

    def await_copy(i):
        if i not in arrived:
            arrived.add(i)
            waiting(i).wait_recv()

    def slots_of(axis):
        n = RING[axis]
        found = []
        for place in range(n):
            d = (place - at[axis] + n) % n
            found.append(jnp.where(d == 0, 0, jnp.where(d <= n // 2, 2 * d - 1, 2 * (n - d))))
        return found

    place_slots = {axis: slots_of(axis) for axis in "yz"}

    def norm(lo):
        chosen = pl.ds(lo, 128)
        x = xs[chosen].astype(jnp.float32)
        scale = lax.rsqrt(jnp.mean(x * x, axis=-1, keepdims=True) + NORM_EPS)
        for tile in range(16):
            z, y = tile // 2, tile % 2 * 2
            weight = sg[z, y, 0, 0]
            for k in range(1, 16):
                weight = weight + sg[z, y + k // 8, k // 2 % 4, k % 2]
            lanes = slice(tile * 128, tile * 128 + 128)
            normed[chosen, lanes] = (x[:, lanes] * scale * weight).astype(jnp.bfloat16)

    lane = lax.broadcasted_iota(jnp.int32, (SEQ, 128), 1)

    def rope(t):
        turned = jnp.where(lane % 64 < 32, pltpu.roll(t, 96, 1), pltpu.roll(t, 32, 1))
        return t * cos[...] + turned * sin[...]

    def features(name, z, lo, n):
        first, second, last = ORDER[name[0]]
        pieces = []
        for y in range(4):
            for x in range(4):
                place = {"x": x, "y": y, "z": z}
                pieces.append(
                    buffers[name][place[last], place[second], place_slots[first][place[first]], :, lo : lo + n]
                )
        return pieces

    def columns(name, lo, n):
        return jnp.concatenate([piece for z in range(8) for piece in features(name, z, lo, n)], axis=0)

    def project_q(name, lo, start):
        t = dot(normed[...], columns(name, lo, 256))
        for s in range(2):
            for half in range(2):
                piece = rope(t[s * SEQ : s * SEQ + SEQ, half * 128 : half * 128 + 128])
                q_all[s * SEQ : s * SEQ + SEQ, start + half * 128 : start + half * 128 + 128] = (
                    piece * HD**-0.5
                ).astype(jnp.bfloat16)

    def project_two(name, start):
        project_q(name, 0, start)
        project_q(name, 256, start + 256)

    def project_kv(lo, turn, low, high):
        t = dot(normed[...], columns("Zp", lo, 256))
        for s in range(2):
            for pair in range(2):
                piece = t[s * SEQ : s * SEQ + SEQ, pair * 128 : pair * 128 + 128]
                if turn:
                    piece = rope(piece)
                moved = pltpu.roll(piece, 64, 1)
                zero = jnp.zeros_like(piece)
                here_rows = slice(s * SEQ, s * SEQ + SEQ)
                for odd in range(2):
                    same, swapped = jnp.where(lane < 64, piece, zero), jnp.where(lane < 64, zero, moved)
                    if odd:
                        same, swapped = jnp.where(lane < 64, moved, zero), jnp.where(lane < 64, zero, piece)
                    low[2 * pair + odd, here_rows] = same.astype(jnp.bfloat16)
                    high[2 * pair + odd, here_rows] = swapped.astype(jnp.bfloat16)

    def attend(s, head):
        here_rows = slice(s * SEQ, s * SEQ + SEQ)
        keys = (k_lo[head, here_rows], k_hi[head, here_rows])
        values = jnp.concatenate([v_lo[head, here_rows], v_hi[head, here_rows]], axis=0)
        for pair in range(2):
            start = head * 256 + pair * 128
            for odd in range(2):
                score[4 * s + 2 * pair + odd] = dot_t(q_all[here_rows, start : start + 128], keys[odd])
        for unit in range(4):
            for block in range(4):
                n = 128 * (block // 2 + 1)
                chosen = slice(block * 64, block * 64 + 64)
                seen = lax.broadcasted_iota(jnp.int32, (64, 128), 1) <= (
                    lax.broadcasted_iota(jnp.int32, (64, 128), 0) + block % 2 * 64
                )
                t = jnp.where(seen, score[4 * s + unit, chosen, n - 128 : n], -1e30)
                if n > 128:
                    t = jnp.concatenate([score[4 * s + unit, chosen, :128], t], axis=1)
                expo = jnp.exp(t - jnp.max(t, axis=-1, keepdims=True))
                share = pl.reciprocal(jnp.sum(expo, axis=-1, keepdims=True), approx=False)
                prob[2 * s + unit // 2, chosen, unit % 2 * SEQ : unit % 2 * SEQ + n] = (expo * share).astype(jnp.bfloat16)
        for pair in range(2):
            start = head * 256 + pair * 128
            ctx[here_rows, start : start + 128] = dot(prob[2 * s + pair], values).astype(jnp.bfloat16)

    def attend_both(head):
        for s in range(2):
            attend(s, head)

    def mix_first(z):
        weights = jnp.concatenate(
            [
                jnp.concatenate(features("Xo", z, 0, 384), axis=0),
                jnp.concatenate(features("Yo", z, 0, 256), axis=0),
            ],
            axis=1,
        )
        acc[z] = dot_t(ctx[:, :640], weights)

    def mix_two(z):
        mix_first(z)
        mix_first(z + 1)

    def chunk_of(k):
        step, way = FAR[k]
        return (at["z"] - way * step + 8) % 8

    def leaving(k):
        return pltpu.make_async_remote_copy(
            src_ref=gone.at[k], dst_ref=come.at[k], send_sem=out_sent.at[k], recv_sem=out_got.at[k],
            device_id=partner, device_id_type=MESH,
        )

    def mix_last(k):
        z = chunk_of(k)
        weights = jnp.concatenate(features("Zo", z, 0, 384), axis=0)
        gone[k] = acc[z, other_rows] + dot_t(ctx[other_rows, 640:], weights)
        mine[k] = acc[z, own_rows] + dot_t(ctx[own_rows, 640:], weights)
        leaving(k).start()

    works = []

    def work(parts, cost, run, *args, needs=()):
        needs = list(needs) + [i for part in parts for i in PART[part]]
        works.append((max(COME[i] for i in needs), cost * 0.7, needs, run, args))

    def prepare():
        starting[7].wait()
        starting[16].wait()
        for copy in tables:
            copy.wait()
        for pair in range(4):
            for odd in range(2):
                prob[pair, :128, odd * SEQ + 128 : odd * SEQ + SEQ] = jnp.zeros((128, 128), jnp.bfloat16)

    work([("G", "g")], 0.0, prepare)
    for lo in range(0, 2 * SEQ, 128):
        work([("G", "g")], 0.2, norm, lo)
    work([("Z", "p")], 0.8, project_kv, 0, True, k_lo, k_hi)
    work([("Z", "p")], 0.8, project_kv, 256, False, v_lo, v_hi)
    for name, start in (("X", 0), ("Y", 512)):
        work([(name, "p")], 1.4, project_two, name + "p", start)
    works[5:] = sorted(works[5:], key=lambda w: w[0])
    for name, heads in (("X", (0, 1)), ("Y", (2, 3))):
        for head in heads:
            work([(name, "p"), ("Z", "p")], 1.7, attend_both, head)
    for z in range(0, 8, 2):
        work([("X", "o"), ("Y", "o")], 0.9, mix_two, z)
    for k in range(8):
        work([], 0.3, mix_last, k, needs=LAST[FAR[k]] if k else [i for i in PART["Z", "o"] if COPIES[i][0][2] < 2])

    now = 0.0
    sending = []

    def do_work():
        nonlocal now
        ready, cost, needs, run, args = works.pop(0)
        for i in needs:
            await_copy(i)
        run(*args)
        now = max(now, ready) + cost

    for begin, i in SENT:
        while works and max(works[0][0], now) + works[0][1] <= begin + 0.3:
            do_work()
        for j in COPIES[i][2]:
            await_copy(j)
        transfer(i).start()
        now = max(now, begin)
        sending.append((begin + COPIES[i][1] / RATE + 3.0, i))
        while sending[0][0] < begin:
            waiting(sending.pop(0)[1]).wait_send()
    while works:
        do_work()
    for i in range(len(COPIES)):
        await_copy(i)

    for k in range(8):
        lanes = pl.ds(pl.multiple_of(chunk_of(k) * 256, 256), 256)
        leaving(k).wait_recv()
        out[:, lanes] = (xs[own_rows, lanes].astype(jnp.float32) + (mine[k] + come[k])).astype(jnp.bfloat16)
    for k in range(8):
        leaving(k).wait_send()
    for _, i in sending:
        waiting(i).wait_send()


def rope_tables():
    position = np.arange(SEQ, dtype=np.float64)
    freq = ROPE_BASE ** (-(np.arange(HD // 2) * 2.0) / HD)
    angle = position[:, None] * freq[None, :]
    cos = np.tile(np.cos(angle), (1, 4))
    sin = np.tile(np.concatenate([-np.sin(angle), np.sin(angle)], axis=1), (1, 2))
    return cos.astype(np.float32), sin.astype(np.float32)


def body(hidden, gain, wq, wk, wv, w_out):
    cos, sin = rope_tables()
    vmem = pltpu.VMEM
    bf16, f32 = jnp.bfloat16, jnp.float32
    n = len(COPIES)
    dma = pltpu.SemaphoreType.DMA
    anywhere = pl.BlockSpec(memory_space=pltpu.HBM)
    inside = pl.BlockSpec(memory_space=pltpu.VMEM)
    return pl.pallas_call(
        kernel,
        out_shape=jax.ShapeDtypeStruct((SEQ, D), bf16),
        in_specs=[anywhere] * 8,
        out_specs=inside,
        scratch_shapes=[
            vmem((4, 4, 8, 16, 512), bf16),
            vmem((4, 4, 8, 16, 512), bf16),
            vmem((8, 4, 4, 16, 512), bf16),
            vmem((4, 4, 8, 16, 384), bf16),
            vmem((4, 4, 8, 16, 256), bf16),
            vmem((8, 4, 4, 16, 384), bf16),
            vmem((8, 4, 4, 2, 1, 128), f32),
            vmem((2 * SEQ, D), bf16),
            vmem((SEQ, 128), f32),
            vmem((SEQ, 128), f32),
            vmem((2 * SEQ, D), bf16),
            vmem((2 * SEQ, 1024), bf16),
            vmem((4, 2 * SEQ, 128), bf16),
            vmem((4, 2 * SEQ, 128), bf16),
            vmem((4, 2 * SEQ, 128), bf16),
            vmem((4, 2 * SEQ, 128), bf16),
            vmem((8, SEQ, SEQ), f32),
            vmem((4, SEQ, 2 * SEQ), bf16),
            vmem((2 * SEQ, 1024), bf16),
            vmem((8, 2 * SEQ, 256), f32),
            vmem((8, SEQ, 256), f32),
            vmem((8, SEQ, 256), f32),
            vmem((8, SEQ, 256), f32),
            vmem((8, 2560), bf16),
            vmem((8,), bf16),
            dma((11,)), dma((8,)), dma((9,)), dma((9,)), dma((n,)), dma((n,)), dma((8,)), dma((8,)),
        ],
        compiler_params=pltpu.CompilerParams(
            collective_id=0, has_side_effects=True, vmem_limit_bytes=40 * 2**20
        ),
        name="attention_block",
    )(*(pltpu.with_memory_space_constraint(a, pltpu.HBM) for a in (hidden, gain, wq, wk, wv, w_out.T, cos, sin)))


def solution(mesh):
    rows = P(("fsdp", "rep"), None)
    placed = (rows, P(("fsdp", "rep")), rows, rows, rows, P(None, ("fsdp", "rep")))
    return jax.shard_map(body, mesh=mesh, in_specs=placed, out_specs=rows, check_vma=False)
```
